256 devices in a mesh: dp: 2 (over x_hi), ep: 128 (over x_lo, z, y, core).
Axes of the slice: x: 4 (x_hi: 2, x_lo: 2; x = x_hi * 2 + x_lo), y: 4, z: 8, core: 2. Of those that a mesh axis runs over, the one named last changes fastest.
Arguments:
- tokens: bfloat16 [65536, 512], P(('dp', 'ep')), parts along dimension 0, may hold values from -6 to 6
- routes: int32 [65536, 2], P(('dp', 'ep')), parts along dimension 0, may hold values from 0 to 127, all different within a row; in each aligned block of 256 rows (0 to 255, 256 to 511, ...) at most 8 rows name the same one
- capacity: int32 [128], replicated, may hold values from 4 to 8, as said below
- expert_in: bfloat16 [128, 512, 2048], P('ep'), may hold values from -0.25 to 0.25
- expert_out: bfloat16 [128, 2048, 512], P('ep'), may hold values from -0.125 to 0.125
- shared_in: bfloat16 [2, 2048, 512], P(None, 'ep'), may hold values from -0.25 to 0.25
- shared_out: bfloat16 [2, 2048, 512], P(None, 'ep'), may hold values from -0.125 to 0.125
- route_gate: bfloat16 [128, 6144], P('ep'), may hold values from -0.25 to 0.25
- shared_gate: bfloat16 [2, 6144], replicated, may hold values from -0.25 to 0.25
Outputs:
- mixed: bfloat16 [65536, 12, 512], P(('dp', 'ep')), parts along dimension 0
The draws below stay inside these ranges and needn't reach their ends.
There are 2 independent parts, one for each index of `dp`. The reference program is written for one: setup_inputs(seed, part) draws one part's arguments, and reference() takes and returns one part's arrays. A program takes and returns all parts, laid end to end along the dimension named above; an argument that names none is the same for every part. Nothing has to cross between parts.
Inputs may be any that keep to these rules, and one draw needn't show every extreme that they name: `routes`: each sample names 2 different experts. Within each device's block of 256 samples no expert is named more than 8 times. `capacity`: some expert accepts exactly 8 rows.
All inputs are finite; a program needn't handle non-finite values.
Results may differ from the reference program's by a relative error of at most 0.0054.
Values may be sent and summed in bfloat16 or wider, within the bound.
A program may use at most 64 MiB of HBM per device.

```python
import math
import jax
import jax.numpy as jnp
import numpy as np
from jax import lax

D = 512
H = 2048
TASKS = 12
SHARED = 2
TOP = 2
TOK_DEV = 256
EXPERTS = 128
CAP = 8
TOKENS = 32768
N_EP = 128


def draw_capacity(key, part):
    first = jax.random.fold_in(key, 11)
    second = jax.random.fold_in(key, 23)
    lowest = max(2, CAP // 2)
    values = jax.random.randint(first, (EXPERTS,), lowest, CAP + 1)
    chosen = jax.random.randint(second, (), 0, EXPERTS)
    return jnp.where(jnp.arange(EXPERTS) == chosen, CAP, values).astype(jnp.int32)


def steps_of(key, extent, pieces, low, high):
    def one(dim, blocks):
        steps = jax.random.uniform(jax.random.fold_in(jax.random.fold_in(key, 6), dim), (blocks,), jnp.float32, low / len(pieces), high / len(pieces))
        return jnp.repeat(jnp.exp(steps), extent[dim] // blocks).reshape((-1,) + (1,) * (len(extent) - dim - 1))

    level = one(*pieces[0])
    for cut in pieces[1:]:
        level = level * one(*cut)
    return level


def deal_out(stream_key, own, number, rows, number_of, top, limit, slope):
    sequence = jax.random.permutation(stream_key, number_of)
    crowded, usual = portions_of(number_of, rows * top, limit, slope, True), portions_of(number_of, rows * top, limit, slope, False)
    places = jnp.arange(number_of)

    def named(tallies, offset_by):
        used = int((tallies > 0).sum())
        fixed = max(1, used // 4)
        passed = fixed + (places - fixed + offset_by * (used - fixed)) % max(1, number_of - fixed)
        return jnp.zeros((number_of,), jnp.int32).at[sequence[jnp.where(places < fixed, places, passed)]].set(jnp.asarray(tallies, jnp.int32))

    tallies = jnp.where(number % 4 == 0, named(crowded, number // 4), named(usual, number - number // 4 - 1))
    mixed = jax.random.permutation(jax.random.fold_in(own, 3), number_of)
    donor, sink = mixed[0:number_of // 2 * 2:2], mixed[1:number_of // 2 * 2:2]
    slack = jnp.minimum(tallies[donor] - 1, limit - tallies[sink]) // 2
    slack = jnp.where((donor == sequence[0]) | (sink == sequence[0]) | (tallies[sink] == 0), 0, jnp.maximum(slack, 0))
    passed = jax.random.randint(jax.random.fold_in(own, 4), (number_of // 2,), 0, 1 << 20) % (slack + 1)
    tallies = tallies.at[donor].add(-passed).at[sink].add(passed)
    members = jnp.searchsorted(jnp.cumsum(tallies), jnp.arange(rows * top), side="right").astype(jnp.int32)
    listing = members.reshape(top, rows).T
    listing = listing[jax.random.permutation(jax.random.fold_in(own, 1), rows)]
    offset_by = jax.random.randint(jax.random.fold_in(own, 2), (rows, 1), 0, top)
    return jnp.take_along_axis(listing, (jnp.arange(top)[None, :] + offset_by) % top, axis=1)


def portions_of(count, total, bound, skew, full):
    weights = [(1 << 20) // math.isqrt(rank ** skew) + 1 for rank in range(1, count + 1)]
    largest = bound if full else min(bound, max(-(-total // count), total * weights[0] // sum(weights)))
    least = 1 if total - largest >= count - 1 else 0
    holding, spare = [largest] + [least] * (count - 1), total - largest - least * (count - 1)
    while spare > 0:
        free = [i for i in range(1, count) if holding[i] < largest] or [i for i in range(1, count) if holding[i] < bound]
        pool, remaining = sum([weights[i] for i in free]), spare
        for i in free:
            more = min(bound - holding[i], max(1, remaining * weights[i] // pool), spare)
            holding[i] = holding[i] + more
            spare = spare - more
    return np.array(holding)


def centred(own_key, shape, width, reach, split=(), kind=jnp.bfloat16):
    gain = steps_of(own_key, shape, split, -0.22, 0.18) if split else 1.0
    entries = jax.random.normal(own_key, shape, jnp.float32) * width * gain
    return jnp.minimum(jnp.maximum(entries, -reach), reach).astype(kind)


def setup_inputs(seed: int = 0, part: int = 0) -> dict:
    keys = jax.random.split(jax.random.key(seed), 10)
    own_keys = jax.random.split(jax.random.fold_in(keys[9], part), 10)
    tokens = centred(own_keys[0], (TOKENS, D), 1.0, 6.0, ((0, 128),))
    routes_keys = jax.random.split(jax.random.fold_in(own_keys[1], 1), TOKENS // TOK_DEV)
    routes_turns = jax.random.permutation(jax.random.fold_in(own_keys[1], 3), TOKENS // TOK_DEV)
    routes = jax.vmap(lambda own, number: deal_out(jax.random.fold_in(own_keys[1], 2), own, number, TOK_DEV, EXPERTS, TOP, CAP, 2))(routes_keys, routes_turns).reshape((TOKENS, TOP))
    capacity = draw_capacity(jax.random.fold_in(keys[9], 71), part)
    expert_in = centred(keys[3], (EXPERTS, D, H), D ** -0.5, 0.25, ((0, 128),))
    expert_out = centred(keys[4], (EXPERTS, H, D), H ** -0.5, 0.125, ((0, 128),))
    shared_in = centred(keys[5], (SHARED, H, D), D ** -0.5, 0.25, ((1, 128),))
    shared_out = centred(keys[6], (SHARED, H, D), H ** -0.5, 0.125, ((1, 128),))
    route_gate = centred(keys[7], (EXPERTS, TASKS * D), D ** -0.5, 0.25, ((0, 128),))
    shared_gate = centred(keys[8], (SHARED, TASKS * D), D ** -0.5, 0.25)
    return dict(tokens=tokens, routes=routes, capacity=capacity, expert_in=expert_in, expert_out=expert_out, shared_in=shared_in, shared_out=shared_out, route_gate=route_gate, shared_gate=shared_gate)


def slot_ranks(routes, capacity):
    blocks = routes.reshape(N_EP, -1)
    chosen = (blocks[:, :, None] == jnp.arange(EXPERTS, dtype=jnp.int32)[None, None, :]).astype(jnp.int32)
    ranked = jnp.sum((jnp.cumsum(chosen, axis=1) - chosen) * chosen, axis=2)
    kept = ranked < capacity[blocks]
    return blocks, ranked.astype(jnp.int32), kept


def reference(tokens, routes, capacity, expert_in, expert_out, shared_in, shared_out, route_gate, shared_gate):
    blocks, ranked, kept = slot_ranks(routes, capacity)
    count = blocks.shape[1]
    owner = jnp.arange(N_EP, dtype=jnp.int32)[:, None]
    position = owner * CAP + ranked
    token_index = owner * TOK_DEV + jnp.arange(count, dtype=jnp.int32)[None, :] // TOP
    flat_slot = blocks * (N_EP * CAP) + position
    target = jnp.where(kept, flat_slot, EXPERTS * N_EP * CAP).reshape(-1)
    source = jnp.full((EXPERTS * N_EP * CAP,), -1, jnp.int32)
    source = source.at[target].set(token_index.reshape(-1), mode="drop").reshape(EXPERTS, N_EP * CAP)

    def serve(item):
        index, w_in, w_out, gate_row = item
        rows = jnp.where(index[:, None] >= 0, tokens[jnp.maximum(index, 0)], jnp.zeros((), tokens.dtype))
        hidden = jax.nn.gelu(jnp.dot(rows, w_in, preferred_element_type=jnp.float32)).astype(jnp.bfloat16)
        out_rows = jnp.dot(hidden, w_out, preferred_element_type=jnp.float32).astype(jnp.bfloat16)
        scores = lax.dot_general(rows, gate_row.reshape(TASKS, D), (((1,), (1,)), ((), ())),
                                 preferred_element_type=jnp.float32).astype(jnp.bfloat16)
        return out_rows, scores

    served, scored = lax.map(serve, (source, expert_in, expert_out, route_gate))
    pick = flat_slot.reshape(-1)
    pair_rows = served.reshape(-1, D)[pick].reshape(N_EP, TOK_DEV, TOP, D)
    pair_scores = scored.reshape(-1, TASKS)[pick].reshape(N_EP, TOK_DEV, TOP, TASKS)
    keep = kept.reshape(N_EP, TOK_DEV, TOP)
    up_full = shared_in.astype(jnp.float32)
    down_full = shared_out.astype(jnp.float32)
    gate_full = shared_gate.reshape(SHARED * TASKS, D)

    def finish(item):
        block, prow, pscore, keep_block = item
        hidden = jax.nn.gelu(jnp.einsum("td,shd->sth", block.astype(jnp.float32), up_full)).astype(jnp.bfloat16)
        shared_rows = jnp.einsum("sth,shd->std", hidden.astype(jnp.float32), down_full)
        shared_logits = lax.dot_general(block, gate_full, (((1,), (1,)), ((), ())),
                                        preferred_element_type=jnp.float32).astype(jnp.bfloat16)
        shared_values = jax.nn.sigmoid(shared_logits.astype(jnp.float32)).reshape(TOK_DEV, SHARED, TASKS)
        routed_values = keep_block.astype(jnp.float32)[:, :, None] * jax.nn.sigmoid(pscore.astype(jnp.float32))
        total = jnp.sum(routed_values, axis=1) + jnp.sum(shared_values, axis=1)
        mixed = jnp.zeros((TOK_DEV, TASKS, D), jnp.float32)
        for k in range(TOP):
            mixed = mixed + (routed_values[:, k] / total)[:, :, None] * prow[:, k].astype(jnp.float32)[:, None, :]
        for s in range(SHARED):
            mixed = mixed + (shared_values[:, s] / total)[:, :, None] * shared_rows[s][:, None, :]
        return mixed.astype(jnp.bfloat16)

    result = lax.map(finish, (tokens.reshape(N_EP, TOK_DEV, D), pair_rows, pair_scores, keep))
    return result.reshape(TOKENS, TASKS, D)
```

```python
import jax
import jax.numpy as jnp
from jax import lax
from jax.experimental import pallas as pl
from jax.experimental.pallas import tpu as pltpu
from jax.sharding import PartitionSpec as P

BF = jnp.bfloat16
F32 = jnp.float32
I32 = jnp.int32
MESH = pl.DeviceIdType.MESH
D = 512
H = 2048
TASKS = 12
TOK = 256
NEP = 128
CH = 4
PER = NEP // CH


def zstep(i):
    return jnp.where(i % 2 == 1, (i + 1) // 2, (8 - i // 2) % 8)


def split_index(me):
    return me // 64, (me // 8) % 8, (me // 2) % 4, me % 2


def join_index(x, z, y, c):
    return ((x * 8 + z) * 4 + y) * 2 + c


def offset_of(n):
    q, r = n // PER, n % PER
    return q % 2, zstep(r % 8), r // 8, q // 2


def ahead(me, n):
    x, z, y, c = split_index(me)
    dx, dz, dy, dc = offset_of(n)
    return join_index(lax.rem(x + dx, 2), lax.rem(z + dz, 8), lax.rem(y + dy, 4), lax.rem(c + dc, 2))


def behind(me, n):
    x, z, y, c = split_index(me)
    dx, dz, dy, dc = offset_of(n)
    return join_index(lax.rem(x + dx, 2), lax.rem(z + 8 - dz, 8), lax.rem(y + 4 - dy, 4), lax.rem(c + dc, 2))


def gelu(x):
    return jax.nn.gelu(x, approximate=True)


def dot(a, b, dims=((1,), (0,))):
    return lax.dot_general(a, b, (dims, ((), ())), preferred_element_type=F32)


def flat_rows(blocks):
    return blocks.astype(F32).reshape(-1, D).astype(BF)


def block_rows(rows):
    return rows.reshape(-1, 8, D).astype(BF)


def gate_tile(rows, group):
    sub = lax.broadcasted_iota(I32, (16, D), 0)
    tiles = []
    for row in rows:
        tile = jnp.zeros((16, D), F32)
        for s in range(TASKS):
            tile = jnp.where(sub == s, row[:, s * D : (s + 1) * D], tile)
        tiles.append(tile)
    zero = jnp.zeros((16, D), F32)
    picked = [zero if group(g) is None else tiles[group(g)] for g in range(8)]
    return jnp.concatenate(picked, axis=0).astype(BF)


def exchange(
    tok_h, routes_h, cap_h, ein_h, eout_h, sin_h, sout_h, rg_h, sg_h,
    rows_o, w_o,
    routes_v, cap_v, rg_v, sg_v, ein_v, eout_v, xs, wbuf, tokq,
    snd, recv, ret, back, lret, lback, sacc, precv, xsend, xrecv, pacc, slog,
    load_sem, big_sem, dsend, drecv, rsend, rrecv, lsend, lrecv,
    tsend, trecv, xssem, xrsem, zsend, zrecv, ysend, yrecv, psend, precv_sem, osend, orecv,
):
    me = lax.axis_index("ep")
    x, z, y, c = split_index(me)

    barrier = pltpu.get_barrier_semaphore()

    @pl.loop(1, NEP)
    def _(i):
        pl.semaphore_signal(barrier, inc=1, device_id={"ep": lax.rem(me + i, NEP)}, device_id_type=MESH)

    def load(src, dst, k):
        return pltpu.make_async_copy(src, dst, load_sem.at[k])

    loads = [
        load(routes_h, routes_v, 0),
        load(cap_h, cap_v, 1),
        load(tok_h, tokq.at[0], 2),
        load(rg_h, rg_v, 3),
        load(sg_h, sg_v, 4),
        load(sin_h.at[x], wbuf.at[0, 0, 0, 0], 5),
        load(sout_h.at[x], wbuf.at[0, 0, 1, 0], 6),
        load(sin_h.at[1 - x], xs.at[0], 7),
        load(sout_h.at[1 - x], xs.at[1], 8),
    ]
    for k in loads:
        k.start()
    big = [
        pltpu.make_async_copy(ein_h.at[0], ein_v, big_sem.at[0]),
        pltpu.make_async_copy(eout_h.at[0], eout_v, big_sem.at[1]),
    ]
    for k in big:
        k.start()
    for k in loads:
        k.wait()

    expert = lax.broadcasted_iota(I32, (NEP, 1), 0)
    ex, ez, ey, ec = expert // 64, (expert // 8) % 8, (expert // 2) % 4, expert % 2
    dz = (ez - z + 8) % 8
    zi = jnp.where(dz == 0, 0, jnp.where(dz <= 4, 2 * dz - 1, 2 * (8 - dz)))
    place = ((((ec - c + 2) % 2) * 2 + (ex - x + 2) % 2) * 4 + (ey - y + 4) % 4) * 8 + zi
    base = (place * 8).astype(F32)
    named = lax.broadcasted_iota(I32, (NEP, TOK), 0)
    chosen = [(named == routes_v[k : k + 1, :]).astype(F32) for k in range(2)]
    earlier = (
        lax.broadcasted_iota(I32, (TOK, TOK), 0) < lax.broadcasted_iota(I32, (TOK, TOK), 1)
    ).astype(BF)
    before = dot((chosen[0] + chosen[1]).astype(BF), earlier)
    cap = jnp.broadcast_to(cap_v[...].astype(F32), (8, NEP)).astype(BF)
    slots = []
    for k in range(2):
        rank = jnp.sum(chosen[k] * before, axis=0, keepdims=True)
        start = jnp.sum(chosen[k] * base, axis=0, keepdims=True)
        limit = dot(cap, chosen[k].astype(BF))[0:1]
        slots.append(jnp.where(rank < limit, start + rank, -1.0))
    slot_row = [s.astype(I32) for s in slots]
    slot_col = [
        jnp.transpose(jnp.broadcast_to(s, (128, TOK)))[:, 0:1].astype(I32) for s in slots
    ]

    own = tokq[0]
    for q in range(CH):
        at = lax.broadcasted_iota(I32, (TOK, TOK), 0) + q * TOK
        pick = jnp.logical_or(at == slot_row[0], at == slot_row[1]).astype(F32).astype(BF)
        rows = block_rows(dot(pick, own))
        snd[pl.ds(q * PER, PER)] = rows
        if q == 0:
            recv[0:1] = rows[0:1]

    gates = gate_tile([rg_v[...].astype(F32)], lambda g: 0)
    sg = sg_v[...].astype(F32)
    sg_own = jnp.where(x == 0, sg[0:1], sg[1:2])
    sg_other = jnp.where(x == 0, sg[1:2], sg[0:1])
    shared_gates = gate_tile([sg_own, sg_other], lambda g: g % 4 - 2 if g % 4 >= 2 else None)
    slog[...] = dot(own, shared_gates, ((1,), (1,))).astype(BF).astype(F32)

    pl.semaphore_wait(barrier, NEP - 1)

    def remote(src, dst, ss, rs, to):
        return pltpu.make_async_remote_copy(
            src_ref=src, dst_ref=dst, send_sem=ss, recv_sem=rs, device_id={"ep": to}, device_id_type=MESH
        )

    def bytes_of(a, sem):
        return pltpu.make_async_copy(a, a, sem)

    across = join_index(1 - x, z, y, c)
    partner = join_index(x, z, y, 1 - c)
    both = join_index(1 - x, z, y, 1 - c)

    for k in range(2):
        remote(xs.at[k], wbuf.at[0, 0, k, 1], xssem.at[k], xrsem.at[k], across).start()

    def dispatch(q):
        @pl.loop(1 if q == 0 else 0, PER)
        def _(r):
            n = q * PER + r
            remote(snd.at[n], recv.at[n], dsend, drecv.at[q], ahead(me, n)).start()

    dispatch(0)
    for p, to in ((1, partner), (2, across), (3, both)):
        remote(tokq.at[0], tokq.at[p], tsend.at[p], trecv.at[p], to).start()
    for k in range(2):
        remote(xs.at[k], wbuf.at[0, 0, k, 1], xssem.at[k], xrsem.at[k], across).wait()

    @pl.loop(1, 8)
    def _(i):
        to = join_index(x, lax.rem(z + zstep(i), 8), y, c)
        remote(wbuf.at[0, 0], wbuf.at[0, i], zsend, zrecv, to).start()

    for q in range(1, CH):
        dispatch(q)
    for k in big:
        k.wait()

    fold = (
        lax.broadcasted_iota(I32, (TOK, 128), 1) // 16 == lax.broadcasted_iota(I32, (TOK, 128), 0) % 8
    )

    def serve(q):
        first = 1 if q == 0 else 0
        got = recv.at[pl.ds(q * PER + first, PER - first)]
        bytes_of(got, drecv.at[q]).wait()
        rows = flat_rows(recv[pl.ds(q * PER, PER)])
        total = jnp.zeros((TOK, D), F32)
        for t in range(4):
            hidden = gelu(dot(rows, ein_v[:, t * 512 : (t + 1) * 512])).astype(BF)
            total = total + dot(hidden, eout_v[t * 512 : (t + 1) * 512, :])
        made = block_rows(total)
        ret[pl.ds(q * PER, PER)] = made
        scores = dot(rows, gates, ((1,), (1,))).astype(BF).astype(F32)
        scores = jnp.sum(
            jnp.where(fold, scores, 0.0).reshape(PER, 8, 128), axis=1, keepdims=True
        )
        lret[pl.ds(q * PER, PER)] = scores
        if q == 0:
            back[0:1] = made[0:1]
            lback[0:1] = scores[0:1]

        @pl.loop(first, PER)
        def _(r):
            n = q * PER + r
            to = behind(me, n)
            remote(ret.at[n], back.at[n], rsend, rrecv.at[q], to).start()
            remote(lret.at[n], lback.at[n], lsend, lrecv, to).start()

    def shared_piece(p):
        up = wbuf[p, :, 0].reshape(256, D)
        down = wbuf[p, :, 1].reshape(256, D)

        @pl.loop(0, 4)
        def _(b):
            hidden = gelu(dot(tokq[b], up, ((1,), (1,)))).astype(BF)
            part = dot(hidden, down)
            if p == 0:
                sacc[b] = part
            else:
                sacc[b] = sacc[b] + part

    serve(0)
    bytes_of(wbuf.at[0, pl.ds(1, 7)], zrecv).wait()
    for dy in (1, 3, 2):
        to = join_index(x, z, lax.rem(y + dy, 4), c)
        remote(wbuf.at[0], wbuf.at[dy], ysend.at[dy], yrecv.at[dy], to).start()
    for p, to in ((1, partner), (2, across), (3, both)):
        remote(tokq.at[0], tokq.at[p], tsend.at[p], trecv.at[p], to).wait()
    shared_piece(0)
    for q in range(1, CH):
        serve(q)
    for dy in (1, 3, 2):
        to = join_index(x, z, lax.rem(y + dy, 4), c)
        remote(wbuf.at[0], wbuf.at[dy], ysend.at[dy], yrecv.at[dy], to).wait()
        shared_piece(dy)
    halves = [remote(sacc.at[1 + 2 * k], precv.at[k], psend.at[k], precv_sem.at[k], partner) for k in range(2)]
    for k in (1, 0):
        halves[k].start()

    def gather(q):
        first = 1 if q == 0 else 0
        bytes_of(back.at[pl.ds(q * PER + first, PER - first)], rrecv.at[q]).wait()
        rows = flat_rows(back[pl.ds(q * PER, PER)])
        at = lax.broadcasted_iota(I32, (TOK, TOK), 1) + q * TOK
        for k in range(2):
            part = dot((at == slot_col[k]).astype(F32).astype(BF), rows)
            if q == 0:
                pacc[k] = part
            else:
                pacc[k] = pacc[k] + part

    gather(0)
    halves[1].wait()
    xsend[...] = (sacc[2] + precv[1]).astype(BF)
    result = remote(xsend, xrecv, osend, orecv, across)
    result.start()
    halves[0].wait()
    rows_o[2] = (sacc[0] + precv[0]).astype(BF)
    for q in range(1, CH):
        gather(q)
    for k in range(2):
        rows_o[k] = pacc[k].astype(BF)
    bytes_of(lback.at[pl.ds(1, NEP - 1)], lrecv).wait()

    scores = lback[...].reshape(NEP, 128).astype(BF)
    lane = lax.broadcasted_iota(I32, (TOK, 128), 1)
    down_i = lax.broadcasted_iota(I32, (128, 128), 0)
    over_i = lax.broadcasted_iota(I32, (128, 128), 1)
    logits = slog[...]
    keep = jnp.ones((TOK, 128), F32)
    for k in range(2):
        col = slot_col[k]
        kept = col >= 0
        spot = jnp.where(kept, col // 8, -1)
        mine = dot((lane == spot).astype(F32).astype(BF), scores)
        mine = jnp.where(lane // 16 == jnp.where(kept, col % 8, -1), mine, 0.0).astype(BF)
        spread = jnp.logical_and(down_i % 16 == over_i % 16, (over_i // 16) % 4 == k)
        logits = logits + dot(mine, spread.astype(F32).astype(BF))
        keep = jnp.where((lane // 16) % 4 == k, kept.astype(F32), keep)
    values = keep * jax.nn.sigmoid(logits)
    pair = values + pltpu.roll(values, 16, 1)
    w_o[...] = values / (pair + pltpu.roll(pair, 32, 1))

    result.wait()
    rows_o[3] = xrecv[...]
    bytes_of(snd.at[pl.ds(1, NEP - 1)], dsend).wait()
    bytes_of(ret.at[pl.ds(1, NEP - 1)], rsend).wait()
    bytes_of(lret.at[pl.ds(1, NEP - 1)], lsend).wait()
    bytes_of(wbuf.at[0, pl.ds(1, 7)], zsend).wait()


def mix(rows_r, w_r, out_r):
    w = w_r[...]
    rows = [rows_r[i].astype(F32) for i in range(4)]
    for s in range(TASKS):
        acc = w[:, s : s + 1] * rows[0]
        for i in range(1, 4):
            acc = acc + w[:, 16 * i + s : 16 * i + s + 1] * rows[i]
        out_r[s] = acc.astype(BF)


def on_device(tokens, routes, capacity, expert_in, expert_out, shared_in, shared_out, route_gate, shared_gate):
    any_space = pl.BlockSpec(memory_space=pltpu.HBM)
    vmem = pl.BlockSpec(memory_space=pltpu.VMEM)
    dma = pltpu.SemaphoreType.DMA
    rows, weights = pl.pallas_call(
        exchange,
        out_shape=(
            jax.ShapeDtypeStruct((4, TOK, D), BF),
            jax.ShapeDtypeStruct((TOK, 128), F32),
        ),
        in_specs=[any_space] * 9,
        out_specs=(vmem, vmem),
        scratch_shapes=[
            pltpu.VMEM((2, TOK), I32),
            pltpu.VMEM((1, NEP), I32),
            pltpu.VMEM((1, TASKS * D), BF),
            pltpu.VMEM((2, TASKS * D), BF),
            pltpu.VMEM((D, H), BF),
            pltpu.VMEM((H, D), BF),
            pltpu.VMEM((2, 16, D), BF),
            pltpu.VMEM((4, 8, 2, 2, 16, D), BF),
            pltpu.VMEM((4, TOK, D), BF),
            pltpu.VMEM((NEP, 8, D), BF),
            pltpu.VMEM((NEP, 8, D), BF),
            pltpu.VMEM((NEP, 8, D), BF),
            pltpu.VMEM((NEP, 8, D), BF),
            pltpu.VMEM((NEP, 1, 128), F32),
            pltpu.VMEM((NEP, 1, 128), F32),
            pltpu.VMEM((4, TOK, D), F32),
            pltpu.VMEM((2, TOK, D), F32),
            pltpu.VMEM((TOK, D), BF),
            pltpu.VMEM((TOK, D), BF),
            pltpu.VMEM((2, TOK, D), F32),
            pltpu.VMEM((TOK, 128), F32),
            dma((9,)),
            dma((2,)),
            dma, dma((CH,)),
            dma, dma((CH,)),
            dma, dma,
            dma((4,)), dma((4,)),
            dma((2,)), dma((2,)),
            dma, dma,
            dma((4,)), dma((4,)),
            dma((2,)), dma((2,)),
            dma, dma,
        ],
        compiler_params=pltpu.CompilerParams(collective_id=0, has_side_effects=True, vmem_limit_bytes=63_000_000),
        name="exchange",
    )(
        tokens, routes.T, capacity.reshape(1, NEP), expert_in, expert_out,
        shared_in, shared_out, route_gate, shared_gate,
    )
    block = 32
    mixed = pl.pallas_call(
        mix,
        out_shape=jax.ShapeDtypeStruct((TASKS, TOK, D), BF),
        grid=(TOK // block,),
        in_specs=[
            pl.BlockSpec((4, block, D), lambda i: (0, i, 0)),
            pl.BlockSpec((block, 128), lambda i: (i, 0)),
        ],
        out_specs=pl.BlockSpec((TASKS, block, D), lambda i: (0, i, 0)),
        name="mix",
    )(rows, weights)
    return mixed.transpose(1, 0, 2)


def solution(mesh):
    rows, experts = P(("dp", "ep"), None), P("ep", None, None)
    return jax.shard_map(
        on_device,
        mesh=mesh,
        in_specs=(rows, rows, P(), experts, experts, P(None, "ep", None), P(None, "ep", None), P("ep", None), P()),
        out_specs=P(("dp", "ep"), None, None),
        check_vma=False,
    )
```

```python
import jax
import jax.numpy as jnp
from jax import lax
from jax.experimental import pallas as pl
from jax.experimental.pallas import tpu as pltpu
from jax.sharding import PartitionSpec as P

BF = jnp.bfloat16
F32 = jnp.float32
I32 = jnp.int32
MESH = pl.DeviceIdType.MESH
D = 512
H = 2048
TASKS = 12
TOK = 256
NEP = 128
CH = 4
PER = NEP // CH
SELF = 2 * PER


ZSTEP = (0, 1, 7, 2, 6, 3, 5, 4)
PARTS = ((0, 1), (1, 4), (5, 3))


def gelu(x):
    return jax.nn.gelu(x, approximate=True)


def dot(a, b, dims=((1,), (0,))):
    return lax.dot_general(a, b, (dims, ((), ())), preferred_element_type=F32)


def flat_rows(blocks):
    return blocks.astype(F32).reshape(-1, D).astype(BF)


def block_rows(rows):
    return rows.reshape(-1, 8, D).astype(BF)


def gate_tile(rows, group):
    sub = lax.broadcasted_iota(I32, (16, D), 0)
    tiles = []
    for row in rows:
        tile = jnp.zeros((16, D), F32)
        for s in range(TASKS):
            tile = jnp.where(sub == s, row[:, s * D : (s + 1) * D], tile)
        tiles.append(tile)
    zero = jnp.zeros((16, D), F32)
    picked = [zero if group(g) is None else tiles[group(g)] for g in range(8)]
    return jnp.concatenate(picked, axis=0).astype(BF)


def exchange(
    tok_h, routes_h, cap_h, ein_h, eout_h, sin_h, sout_h, rg_h, sg_h,
    rows_o, w_o,
    routes_v, cap_v, rg_v, sg_v, ein_v, eout_v, xs, wbuf, tokq,
    snd, recv, ret, back, lret, lback, sacc, precv, xsend, xrecv, pacc, slog,
    load_sem, big_sem, dsend, drecv, rsend, rrecv, lsend, lrecv,
    tsend, trecv, xssem, xrsem, zsend, zrecv, ysend, yrecv, psend, precv_sem, osend, orecv, csend, crecv,
):
    me = lax.axis_index("ep")
    x, z, y, c = me >> 6, (me >> 3) & 7, (me >> 1) & 3, me & 1
    d = lax.axis_index("dp")
    mine = x ^ d
    xpart = [x * 64, (1 - x) * 64]
    zpart = [((z + d) & 7) * 8 for d in range(8)]
    cpart = [c, 1 - c]

    def load(src, dst, k):
        return pltpu.make_async_copy(src, dst, load_sem.at[k])

    loads = [
        load(routes_h, routes_v, 0),
        load(cap_h, cap_v, 1),
        load(tok_h, tokq.at[0], 2),
        load(rg_h, rg_v, 3),
        load(sg_h, sg_v, 4),
        load(sin_h, xs.at[0], 5),
        load(sout_h, xs.at[1], 6),
    ]
    for k in loads:
        k.start()
    big = [
        pltpu.make_async_copy(ein_h.at[0], ein_v, big_sem.at[0]),
        pltpu.make_async_copy(eout_h.at[0], eout_v, big_sem.at[1]),
    ]
    for k in big:
        k.start()

    barrier = pltpu.get_barrier_semaphore()
    other = {"dp": 1 - d, "ep": xpart[1] + (me & 63)}
    pl.semaphore_signal(barrier, inc=1, device_id=other, device_id_type=MESH)
    for dz in (4, 3, 5, 2, 6, 1, 7, 0):
        for dy in (2, 1, 3, 0):
            for dx in (1, 0):
                for dc in (1, 0):
                    if dz or dy or dx or dc:
                        to = xpart[dx] + zpart[dz] + ((y + dy) & 3) * 2 + cpart[dc]
                        pl.semaphore_signal(barrier, inc=1, device_id={"ep": to}, device_id_type=MESH)

    with jax.named_scope("loadwait"):
        for k in loads:
            k.wait()

    expert = lax.broadcasted_iota(I32, (NEP, 1), 0)
    dz = ((expert >> 3) - z + 8) & 7
    zi = jnp.where(dz == 0, 0, jnp.where(dz <= 4, 2 * dz - 1, 2 * (8 - dz)))
    place = (((((expert - c + 2) & 1) + 2 - 2 * (((expert >> 6) - x + 2) & 1)) * 4) + (((expert >> 1) - y + 4) & 3)) * 8 + zi
    base = (place * 8).astype(F32)
    named = lax.broadcasted_iota(I32, (NEP, TOK), 0)
    chosen = [(named == routes_v[k : k + 1, :]).astype(F32) for k in range(2)]
    earlier = (
        lax.broadcasted_iota(I32, (TOK, TOK), 0) < lax.broadcasted_iota(I32, (TOK, TOK), 1)
    ).astype(BF)
    before = dot((chosen[0] + chosen[1]).astype(BF), earlier)
    cap = jnp.broadcast_to(cap_v[...].astype(F32), (8, NEP)).astype(BF)
    slots = []
    for k in range(2):
        rank = jnp.sum(chosen[k] * before, axis=0, keepdims=True)
        start = jnp.sum(chosen[k] * base, axis=0, keepdims=True)
        limit = dot(cap, chosen[k].astype(BF))[0:1]
        slots.append(jnp.where(rank < limit, start + rank, -1.0))
    slot_row = [s.astype(I32) for s in slots]
    slot_col = [
        jnp.transpose(jnp.broadcast_to(s, (128, TOK)))[:, 0:1].astype(I32) for s in slots
    ]

    own = tokq[0]
    for q in range(CH):
        at = lax.broadcasted_iota(I32, (TOK, TOK), 0) + q * TOK
        pick = jnp.logical_or(at == slot_row[0], at == slot_row[1]).astype(F32).astype(BF)
        rows = block_rows(dot(pick, own))
        snd[pl.ds(q * PER, PER)] = rows
        if q == SELF // PER:
            recv[SELF : SELF + 1] = rows[0:1]

    wbuf[d, 0, 0, x] = xs[d, mine]
    gates = gate_tile([rg_v[...].astype(F32)], lambda g: 0)
    sg = sg_v[...].astype(F32)
    sg_own = jnp.where(mine == 0, sg[0:1], sg[1:2])
    sg_other = jnp.where(mine == 0, sg[1:2], sg[0:1])
    shared_gates = gate_tile([sg_own, sg_other], lambda g: g % 4 - 2 if g % 4 >= 2 else None)
    slog[...] = dot(own, shared_gates, ((1,), (1,))).astype(BF).astype(F32)

    with jax.named_scope("barrier"):
        pl.semaphore_wait(barrier, NEP)

    def remote(src, dst, ss, rs, to):
        return pltpu.make_async_remote_copy(
            src_ref=src, dst_ref=dst, send_sem=ss, recv_sem=rs,
            device_id=to if isinstance(to, dict) else {"ep": to}, device_id_type=MESH,
        )

    def bytes_of(a, sem):
        return pltpu.make_async_copy(a, a, sem)

    def toward(dx, dz, dy, dc):
        return xpart[dx] + zpart[dz] + ((y + dy) & 3) * 2 + cpart[dc]

    def each(q, low, high, sign, act):
        dx, dc = 1 - q // 2, q % 2
        if q == SELF // PER and low == 0:
            for i in range(1, 8):
                act(SELF + i, toward(dx, sign * ZSTEP[i] % 8, 0, dc))
            low = 1

        @pl.loop(low, high)
        def _(dy):
            for i in range(8):
                act(q * PER + dy * 8 + i, toward(dx, sign * ZSTEP[i] % 8, 4 + sign * dy, dc))

    across = toward(1, 0, 0, 0)
    partner = toward(0, 0, 0, 1)

    def dispatch(q, low=0, high=4):
        each(q, low, high, 1, lambda n, to: remote(snd.at[n], recv.at[n], dsend, drecv.at[q], to).start())

    x_half = remote(xs.at[d, 1 - mine], wbuf.at[d, 0, 0, x], xssem, xrsem, across)
    x_half.start()
    dispatch(0, 0, 2)
    with jax.named_scope("xwait"):
        x_half.wait()

    def along_z(src, slot, k, dz):
        return remote(src, wbuf.at[(d, 0) + slot], zsend.at[k], zrecv.at[k], toward(0, dz, 0, 0))

    near = [along_z(wbuf.at[d, 0, 0], (i,), i, ZSTEP[i]) for i in (1, 2, 3, 4)]
    far = [
        along_z(wbuf.at[d, 0, 3], (5,), 5, 1),
        along_z(wbuf.at[d, 0, 4], (6,), 6, 7),
        along_z(wbuf.at[d, 0, 3, 0], (7, 0), 0, 2),
        along_z(wbuf.at[d, 0, 4, 1], (7, 1), 7, 6),
    ]
    along_y = []
    for j, (first, count) in enumerate(PARTS):
        along_y.append({
            dy: remote(
                wbuf.at[d, 0, pl.ds(first, count)], wbuf.at[d, dy, pl.ds(first, count)],
                ysend.at[dy, j], yrecv.at[dy, j], toward(0, 0, dy, 0),
            )
            for dy in (1, 3, 2)
        })
    swap = [remote(wbuf.at[d, p], wbuf.at[d, p], csend.at[p], crecv.at[p], other) for p in range(4)]
    quad = [
        remote(tokq.at[0], tokq.at[p], tsend.at[p], trecv.at[p], to)
        for p, to in ((1, partner), (2, across))
    ]
    passed_on = remote(tokq.at[2], tokq.at[3], tsend.at[3], trecv.at[3], partner)

    for k in near:
        k.start()
    for k in along_y[0].values():
        k.start()
    dispatch(0, 2, 4)
    with jax.named_scope("nearwait"):
        for k in near:
            k.wait_recv()
    for k in far:
        k.start()
    for k in along_y[1].values():
        k.start()
    with jax.named_scope("dispatch123"):
        dispatch(1)
        for k in quad:
            k.start()
        dispatch(2)
        dispatch(3)
    for k in big:
        k.wait()

    fold = (
        lax.broadcasted_iota(I32, (TOK, 128), 1) // 16 == lax.broadcasted_iota(I32, (TOK, 128), 0) % 8
    )

    def serve(q):
        first = 1 if q == SELF // PER else 0
        with jax.named_scope("dwait"):
            bytes_of(recv.at[pl.ds(q * PER + first, PER - first)], drecv.at[q]).wait()
        rows = flat_rows(recv[pl.ds(q * PER, PER)])
        scores = dot(rows, gates, ((1,), (1,))).astype(BF).astype(F32)
        scores = jnp.sum(
            jnp.where(fold, scores, 0.0).reshape(PER, 8, 128), axis=1, keepdims=True
        )
        lret[pl.ds(q * PER, PER)] = scores
        if q == SELF // PER:
            lback[SELF : SELF + 1] = scores[0:1]
        total = jnp.zeros((TOK, D), F32)
        for t in range(4):
            hidden = gelu(dot(rows, ein_v[:, t * 512 : (t + 1) * 512])).astype(BF)
            total = total + dot(hidden, eout_v[t * 512 : (t + 1) * 512, :])
        made = block_rows(total)
        ret[pl.ds(q * PER, PER)] = made
        if q == SELF // PER:
            back[SELF : SELF + 1] = made[0:1]
        with jax.named_scope("logsend"):
            each(q, 0, 4, -1, lambda n, to: remote(lret.at[n], lback.at[n], lsend, lrecv, to).start())
        with jax.named_scope("retsend"):
            each(q, 0, 4, -1, lambda n, to: remote(ret.at[n], back.at[n], rsend, rrecv.at[q], to).start())

    def shared_block(p, b, up, down):
        hidden = gelu(dot(tokq[b], up, ((1,), (1,)))).astype(BF)
        part = dot(hidden, down)
        if p == 0:
            sacc[b] = part
        else:
            sacc[b] = sacc[b] + part

    def shared_weights(p):
        with jax.named_scope("swapwait"):
            swap[p].wait()
        return wbuf[0, p].reshape(256, D), wbuf[1, p].reshape(256, D)

    def shared_piece(p):
        up, down = shared_weights(p)

        @pl.loop(0, 4)
        def _(b):
            shared_block(p, b, up, down)

    def y_arrived(dy):
        with jax.named_scope("ywait"):
            for part in along_y:
                part[dy].wait()
        swap[dy].start()

    serve(0)
    with jax.named_scope("farwait"):
        for k in far:
            k.wait_recv()
    for k in along_y[2].values():
        k.start()
    swap[0].start()
    serve(1)
    with jax.named_scope("quadwait"):
        for k in quad:
            k.wait()
        passed_on.start()
    y_arrived(1)
    y_arrived(3)
    serve(2)
    passed_on.wait()
    shared_piece(0)
    y_arrived(2)
    serve(3)
    shared_piece(1)
    shared_piece(3)
    up, down = shared_weights(2)
    halves = [remote(sacc.at[1 + 2 * k], precv.at[k], psend.at[k], precv_sem.at[k], partner) for k in range(2)]
    result = remote(xsend, xrecv, osend, orecv, across)
    shared_block(2, 3, up, down)
    halves[1].start()
    shared_block(2, 1, up, down)
    halves[0].start()
    shared_block(2, 2, up, down)
    with jax.named_scope("h1wait"):
        halves[1].wait()
    xsend[...] = (sacc[2] + precv[1]).astype(BF)
    result.start()
    shared_block(2, 0, up, down)
    with jax.named_scope("h0wait"):
        halves[0].wait()
    rows_o[2] = (sacc[0] + precv[0]).astype(BF)

    def gather(q):
        first = 1 if q == SELF // PER else 0
        with jax.named_scope("rwait"):
            bytes_of(back.at[pl.ds(q * PER + first, PER - first)], rrecv.at[q]).wait()
        rows = flat_rows(back[pl.ds(q * PER, PER)])
        at = lax.broadcasted_iota(I32, (TOK, TOK), 1) + q * TOK
        for k in range(2):
            part = dot((at == slot_col[k]).astype(F32).astype(BF), rows)
            if q == 0:
                pacc[k] = part
            elif q < CH - 1:
                pacc[k] = pacc[k] + part
            else:
                rows_o[k] = (pacc[k] + part).astype(BF)

    for q in range(CH - 1):
        gather(q)
    with jax.named_scope("lwait"):
        bytes_of(lback.at[pl.ds(1, NEP - 1)], lrecv).wait()

    scores = lback[...].reshape(NEP, 128).astype(BF)
    lane = lax.broadcasted_iota(I32, (TOK, 128), 1)
    down_i = lax.broadcasted_iota(I32, (128, 128), 0)
    over_i = lax.broadcasted_iota(I32, (128, 128), 1)
    logits = slog[...]
    keep = jnp.ones((TOK, 128), F32)
    for k in range(2):
        col = slot_col[k]
        kept = col >= 0
        spot = jnp.where(kept, col // 8, -1)
        mine = dot((lane == spot).astype(F32).astype(BF), scores)
        mine = jnp.where(lane // 16 == jnp.where(kept, col % 8, -1), mine, 0.0).astype(BF)
        spread = jnp.logical_and(down_i % 16 == over_i % 16, (over_i // 16) % 4 == k)
        logits = logits + dot(mine, spread.astype(F32).astype(BF))
        keep = jnp.where((lane // 16) % 4 == k, kept.astype(F32), keep)
    values = keep * jax.nn.sigmoid(logits)
    pair = values + pltpu.roll(values, 16, 1)
    w_o[...] = values / (pair + pltpu.roll(pair, 32, 1))

    with jax.named_scope("owait"):
        result.wait()
    rows_o[3] = xrecv[...]
    gather(CH - 1)
    for k in near + far:
        k.wait_send()
    bytes_of(snd.at[pl.ds(1, NEP - 1)], dsend).wait()
    bytes_of(lret.at[pl.ds(1, NEP - 1)], lsend).wait()
    bytes_of(ret.at[pl.ds(1, NEP - 1)], rsend).wait()


TB = 32
OUT_PARTS = 8


def mix(rows_r, w_r, out_h, buf, sem):
    wide = 4 * TB
    w = w_r[...]
    high = w.astype(BF)
    lane = lax.broadcasted_iota(I32, (128, TASKS * wide), 1)
    row = lax.broadcasted_iota(I32, (128, TASKS * wide), 0)
    take = (row == (lane % wide) // TB * 16 + lane // wide).astype(F32).astype(BF)
    diagonal = (
        lax.broadcasted_iota(I32, (TOK, wide), 1) % TB == lax.broadcasted_iota(I32, (TOK, wide), 0) % TB
    )
    planes = []
    for source in (high, (w - high.astype(F32)).astype(BF)):
        spread = dot(source, take)
        planes.append([
            jnp.where(diagonal, spread[:, s * wide : (s + 1) * wide], 0.0).astype(BF) for s in range(TASKS)
        ])
    size = TOK // OUT_PARTS

    def put(h):
        at = pl.ds(h * size, size)
        return pltpu.make_async_copy(buf.at[:, at], out_h.at[:, at], sem.at[h])

    for b in range(TOK // TB):
        at = slice(b * TB, (b + 1) * TB)
        terms = jnp.concatenate([rows_r[i, at] for i in range(4)] * 2, axis=0)
        left = jnp.concatenate(
            [jnp.concatenate([planes[0][s][at] for s in range(TASKS)], axis=0),
             jnp.concatenate([planes[1][s][at] for s in range(TASKS)], axis=0)], axis=1)
        made = dot(left, terms).astype(BF)
        for s in range(TASKS):
            buf[s, at] = made[s * TB : (s + 1) * TB]
        if (b + 1) * TB % size == 0:
            put((b + 1) * TB // size - 1).start()
    for h in range(OUT_PARTS):
        put(h).wait()


def on_device(tokens, routes, capacity, expert_in, expert_out, shared_in, shared_out, route_gate, shared_gate):
    hbm = pl.BlockSpec(memory_space=pltpu.HBM)
    vmem = pl.BlockSpec(memory_space=pltpu.VMEM)
    dma = pltpu.SemaphoreType.DMA
    rows, weights = pl.pallas_call(
        exchange,
        out_shape=(
            jax.ShapeDtypeStruct((4, TOK, D), BF),
            jax.ShapeDtypeStruct((TOK, 128), F32),
        ),
        in_specs=[hbm] * 9,
        out_specs=(vmem, vmem),
        scratch_shapes=[
            pltpu.VMEM((2, TOK), I32),
            pltpu.VMEM((1, NEP), I32),
            pltpu.VMEM((1, TASKS * D), BF),
            pltpu.VMEM((2, TASKS * D), BF),
            pltpu.VMEM((D, H), BF),
            pltpu.VMEM((H, D), BF),
            pltpu.VMEM((2, 2, 16, D), BF),
            pltpu.VMEM((2, 4, 8, 2, 16, D), BF),
            pltpu.VMEM((4, TOK, D), BF),
            pltpu.VMEM((NEP, 8, D), BF),
            pltpu.VMEM((NEP, 8, D), BF),
            pltpu.VMEM((NEP, 8, D), BF),
            pltpu.VMEM((NEP, 8, D), BF),
            pltpu.VMEM((NEP, 1, 128), F32),
            pltpu.VMEM((NEP, 1, 128), F32),
            pltpu.VMEM((4, TOK, D), F32),
            pltpu.VMEM((2, TOK, D), F32),
            pltpu.VMEM((TOK, D), BF),
            pltpu.VMEM((TOK, D), BF),
            pltpu.VMEM((2, TOK, D), F32),
            pltpu.VMEM((TOK, 128), F32),
            dma((7,)),
            dma((2,)),
            dma, dma((CH,)),
            dma, dma((CH,)),
            dma, dma,
            dma((4,)), dma((4,)),
            dma, dma,
            dma((8,)), dma((8,)),
            dma((4, 3)), dma((4, 3)),
            dma((2,)), dma((2,)),
            dma, dma,
            dma((4,)), dma((4,)),
        ],
        compiler_params=pltpu.CompilerParams(collective_id=0, has_side_effects=True, vmem_limit_bytes=40 * 2**20),
        name="exchange",
    )(*[
        pltpu.with_memory_space_constraint(a, pltpu.HBM)
        for a in (
            tokens, routes.T, capacity.reshape(1, NEP), expert_in, expert_out,
            shared_in, shared_out, route_gate, shared_gate,
        )
    ])
    mixed = pl.pallas_call(
        mix,
        out_shape=jax.ShapeDtypeStruct((TASKS, TOK, D), BF),
        in_specs=[vmem, vmem],
        out_specs=hbm,
        scratch_shapes=[pltpu.VMEM((TASKS, TOK, D), BF), dma((OUT_PARTS,))],
        compiler_params=pltpu.CompilerParams(vmem_limit_bytes=24 * 2**20),
        name="mix",
    )(rows, weights)
    return mixed.transpose(1, 0, 2)


def solution(mesh):
    rows, experts = P(("dp", "ep"), None), P("ep", None, None)
    return jax.shard_map(
        on_device,
        mesh=mesh,
        in_specs=(rows, rows, P(), experts, experts, P(None, "ep", None), P(None, "ep", None), P("ep", None), P()),
        out_specs=P(("dp", "ep"), None, None),
        check_vma=False,
    )
```

```python
import jax
import jax.numpy as jnp
from jax import lax
from jax.experimental import pallas as pl
from jax.experimental.pallas import tpu as pltpu
from jax.sharding import PartitionSpec as P

BF = jnp.bfloat16
F32 = jnp.float32
I32 = jnp.int32
MESH = pl.DeviceIdType.MESH
D = 512
H = 2048
TASKS = 12
TOK = 256
NEP = 128
CH = 4
PER = NEP // CH
SELF = 2 * PER


TB = 32
ZSTEP = (0, 1, 7, 2, 6, 3, 5, 4)
PARTS = ((0, 1), (1, 4), (5, 3))


def gelu(x):
    return jax.nn.gelu(x, approximate=True)


def dot(a, b, dims=((1,), (0,))):
    return lax.dot_general(a, b, (dims, ((), ())), preferred_element_type=F32)


def flat_rows(blocks):
    return blocks.astype(F32).reshape(-1, D).astype(BF)


def block_rows(rows):
    return rows.reshape(-1, 8, D).astype(BF)


def gate_tile(rows, group):
    sub = lax.broadcasted_iota(I32, (16, D), 0)
    tiles = []
    for row in rows:
        tile = jnp.zeros((16, D), F32)
        for s in range(TASKS):
            tile = jnp.where(sub == s, row[:, s * D : (s + 1) * D], tile)
        tiles.append(tile)
    zero = jnp.zeros((16, D), F32)
    picked = [zero if group(g) is None else tiles[group(g)] for g in range(8)]
    return jnp.concatenate(picked, axis=0).astype(BF)


def exchange(
    tok_h, routes_h, cap_h, ein_h, eout_h, sin_h, sout_h, rg_h, sg_h,
    rows_o, w_o,
    routes_v, cap_v, rg_v, sg_v, ein_v, eout_v, xs, wbuf, tokq,
    snd, recv, ret, back, lret, lback, sacc, precv, xsend, xrecv, pacc, slog,
    load_sem, big_sem, dsend, drecv, rsend, rrecv, lsend, lrecv,
    tsend, trecv, xssem, xrsem, zsend, zrecv, ysend, yrecv, psend, precv_sem, osend, orecv, csend, crecv,
):
    me = lax.axis_index("ep")
    x, z, y, c = me >> 6, (me >> 3) & 7, (me >> 1) & 3, me & 1
    d = lax.axis_index("dp")
    mine = x ^ d
    xpart = [x * 64, (1 - x) * 64]
    zpart = [((z + d) & 7) * 8 for d in range(8)]
    cpart = [c, 1 - c]

    def load(src, dst, k):
        return pltpu.make_async_copy(src, dst, load_sem.at[k])

    loads = [
        load(routes_h, routes_v, 0),
        load(cap_h, cap_v, 1),
        load(tok_h, tokq.at[0], 2),
        load(rg_h, rg_v, 3),
        load(sg_h, sg_v, 4),
    ]
    for k in loads:
        k.start()
    load(sin_h, xs.at[0], 5).start()
    load(sout_h, xs.at[1], 5).start()
    big = [
        pltpu.make_async_copy(ein_h.at[0], ein_v, big_sem.at[0]),
        pltpu.make_async_copy(eout_h.at[0], eout_v, big_sem.at[1]),
    ]
    for k in big:
        k.start()

    barrier = pltpu.get_barrier_semaphore()
    other = {"dp": 1 - d, "ep": xpart[1] + (me & 63)}
    pl.semaphore_signal(barrier, inc=1, device_id=other, device_id_type=MESH)
    for dz in (4, 3, 5, 2, 6, 1, 7, 0):
        for dy in (2, 1, 3, 0):
            for dx in (1, 0):
                for dc in (1, 0):
                    if dz or dy or dx or dc:
                        to = xpart[dx] + zpart[dz] + ((y + dy) & 3) * 2 + cpart[dc]
                        pl.semaphore_signal(barrier, inc=1, device_id={"ep": to}, device_id_type=MESH)

    with jax.named_scope("loadwait"):
        for k in loads:
            k.wait()
        load(xs, xs, 5).wait()

    expert = lax.broadcasted_iota(I32, (NEP, 1), 0)
    dz = ((expert >> 3) - z + 8) & 7
    zi = jnp.where(dz == 0, 0, jnp.where(dz <= 4, 2 * dz - 1, 2 * (8 - dz)))
    place = (((((expert - c + 2) & 1) + 2 - 2 * (((expert >> 6) - x + 2) & 1)) * 4) + (((expert >> 1) - y + 4) & 3)) * 8 + zi
    base = (place * 8).astype(F32)
    named = lax.broadcasted_iota(I32, (NEP, TOK), 0)
    chosen = [(named == routes_v[k : k + 1, :]).astype(F32) for k in range(2)]
    earlier = (
        lax.broadcasted_iota(I32, (TOK, TOK), 0) < lax.broadcasted_iota(I32, (TOK, TOK), 1)
    ).astype(BF)
    before = dot((chosen[0] + chosen[1]).astype(BF), earlier)
    cap = jnp.broadcast_to(cap_v[...].astype(F32), (8, NEP)).astype(BF)
    slots = []
    for k in range(2):
        rank = jnp.sum(chosen[k] * before, axis=0, keepdims=True)
        start = jnp.sum(chosen[k] * base, axis=0, keepdims=True)
        limit = dot(cap, chosen[k].astype(BF))[0:1]
        slots.append(jnp.where(rank < limit, start + rank, -1.0))
    slot_row = [s.astype(I32) for s in slots]
    slot_col = [
        jnp.transpose(jnp.broadcast_to(s, (128, TOK)))[:, 0:1].astype(I32) for s in slots
    ]

    own = tokq[0]
    for q in range(CH):
        at = lax.broadcasted_iota(I32, (TOK, TOK), 0) + q * TOK
        pick = jnp.logical_or(at == slot_row[0], at == slot_row[1]).astype(F32).astype(BF)
        rows = block_rows(dot(pick, own))
        snd[pl.ds(q * PER, PER)] = rows
        if q == SELF // PER:
            recv[SELF : SELF + 1] = rows[0:1]

    wbuf[d, 0, 0, x] = xs[d, mine]
    gates = gate_tile([rg_v[...].astype(F32)], lambda g: 0)
    sg = sg_v[...].astype(F32)
    sg_own = jnp.where(mine == 0, sg[0:1], sg[1:2])
    sg_other = jnp.where(mine == 0, sg[1:2], sg[0:1])
    shared_gates = gate_tile([sg_own, sg_other], lambda g: g % 4 - 2 if g % 4 >= 2 else None)
    slog[...] = dot(own, shared_gates, ((1,), (1,))).astype(BF).astype(F32)

    with jax.named_scope("barrier"):
        pl.semaphore_wait(barrier, NEP)

    def remote(src, dst, ss, rs, to):
        return pltpu.make_async_remote_copy(
            src_ref=src, dst_ref=dst, send_sem=ss, recv_sem=rs,
            device_id=to if isinstance(to, dict) else {"ep": to}, device_id_type=MESH,
        )

    def bytes_of(a, sem):
        return pltpu.make_async_copy(a, a, sem)

    def toward(dx, dz, dy, dc):
        return xpart[dx] + zpart[dz] + ((y + dy) & 3) * 2 + cpart[dc]

    def each(q, low, high, sign, act):
        dx, dc = 1 - q // 2, q % 2
        if q == SELF // PER and low == 0:
            for i in range(1, 8):
                act(SELF + i, toward(dx, sign * ZSTEP[i] % 8, 0, dc))
            low = 1

        @pl.loop(low, high)
        def _(dy):
            for i in range(8):
                act(q * PER + dy * 8 + i, toward(dx, sign * ZSTEP[i] % 8, 4 + sign * dy, dc))

    across = toward(1, 0, 0, 0)
    partner = toward(0, 0, 0, 1)

    def dispatch(q, low=0, high=4):
        each(q, low, high, 1, lambda n, to: remote(snd.at[n], recv.at[n], dsend, drecv.at[q], to).start())

    x_half = remote(xs.at[d, 1 - mine], wbuf.at[d, 0, 0, x], xssem, xrsem, across)
    x_half.start()
    dispatch(0, 0, 2)
    with jax.named_scope("xwait"):
        x_half.wait()

    def along_z(src, slot, k, dz):
        return remote(src, wbuf.at[(d, 0) + slot], zsend, zrecv.at[k], toward(0, dz, 0, 0))

    near = [along_z(wbuf.at[d, 0, 0], (i,), 0, ZSTEP[i]) for i in (1, 2, 3, 4)]
    far = [
        along_z(wbuf.at[d, 0, 3], (5,), 1, 1),
        along_z(wbuf.at[d, 0, 4], (6,), 1, 7),
        along_z(wbuf.at[d, 0, 3, 0], (7, 0), 1, 2),
        along_z(wbuf.at[d, 0, 4, 1], (7, 1), 1, 6),
    ]
    along_y = []
    for j, (first, count) in enumerate(PARTS):
        along_y.append({
            dy: remote(
                wbuf.at[d, 0, pl.ds(first, count)], wbuf.at[d, dy, pl.ds(first, count)],
                ysend, yrecv.at[j], toward(0, 0, dy, 0),
            )
            for dy in (1, 3, 2)
        })
    swap = []
    for j, (first, count) in enumerate(PARTS):
        swap.append([
            remote(
                wbuf.at[d, p, pl.ds(first, count)], wbuf.at[d, p, pl.ds(first, count)],
                csend, crecv.at[p], other,
            )
            for p in range(4)
        ])
    quad = [
        remote(tokq.at[0], tokq.at[p], tsend, trecv.at[0], to)
        for p, to in ((1, partner), (2, across))
    ]
    passed_on = remote(tokq.at[2], tokq.at[3], tsend, trecv.at[1], partner)

    def y_arrived(j):
        with jax.named_scope("ywait"):
            first, count = PARTS[j]
            bytes_of(wbuf.at[d, pl.ds(1, 3), pl.ds(first, count)], yrecv.at[j]).wait()
        for dy in (1, 3, 2):
            swap[j][dy].start()

    for k in near:
        k.start()
    for k in along_y[0].values():
        k.start()
    swap[0][0].start()
    dispatch(0, 2, 4)
    dispatch(1, 0, 2)
    with jax.named_scope("nearwait"):
        bytes_of(wbuf.at[d, 0, pl.ds(1, 4)], zrecv.at[0]).wait()
    for k in far:
        k.start()
    for k in along_y[1].values():
        k.start()
    swap[1][0].start()
    dispatch(1, 2, 4)
    for k in quad:
        k.start()
    with jax.named_scope("farwait"):
        bytes_of(wbuf.at[d, 0, pl.ds(5, 3)], zrecv.at[1]).wait()
    for k in along_y[2].values():
        k.start()
    swap[2][0].start()
    dispatch(2)
    dispatch(3)
    y_arrived(0)
    for k in big:
        k.wait()

    fold = (
        lax.broadcasted_iota(I32, (TOK, 128), 1) // 16 == lax.broadcasted_iota(I32, (TOK, 128), 0) % 8
    )

    def serve(q):
        first = 1 if q == SELF // PER else 0
        with jax.named_scope("dwait"):
            bytes_of(recv.at[pl.ds(q * PER + first, PER - first)], drecv.at[q]).wait()
        rows = flat_rows(recv[pl.ds(q * PER, PER)])
        scores = dot(rows, gates, ((1,), (1,))).astype(BF).astype(F32)
        scores = jnp.sum(
            jnp.where(fold, scores, 0.0).reshape(PER, 8, 128), axis=1, keepdims=True
        )
        lret[pl.ds(q * PER, PER)] = scores
        if q == SELF // PER:
            lback[SELF : SELF + 1] = scores[0:1]
        total = jnp.zeros((TOK, D), F32)
        for t in range(4):
            hidden = gelu(dot(rows, ein_v[:, t * 512 : (t + 1) * 512])).astype(BF)
            total = total + dot(hidden, eout_v[t * 512 : (t + 1) * 512, :])
        made = block_rows(total)
        ret[pl.ds(q * PER, PER)] = made
        if q == SELF // PER:
            back[SELF : SELF + 1] = made[0:1]
        with jax.named_scope("logsend"):
            each(q, 0, 4, -1, lambda n, to: remote(lret.at[n], lback.at[n], lsend, lrecv, to).start())
        with jax.named_scope("retsend"):
            if q < CH - 1:
                each(q, 0, 4, -1, lambda n, to: remote(ret.at[n], back.at[n], rsend, rrecv.at[q], to).start())
            else:
                for i in (7, 6, 5, 4, 3, 2, 1, 0):
                    for dy in (2, 1, 3, 0):
                        n = q * PER + dy * 8 + i
                        to = toward(1 - q // 2, -ZSTEP[i] % 8, 4 - dy, q % 2)
                        remote(ret.at[n], back.at[n], rsend, rrecv.at[q], to).start()

    def shared_block(p, b, up, down):
        hidden = gelu(dot(tokq[b], up, ((1,), (1,)))).astype(BF)
        part = dot(hidden, down)
        if p == 0:
            sacc[b] = part
        else:
            sacc[b] = sacc[b] + part

    def shared_weights(p):
        with jax.named_scope("swapwait"):
            bytes_of(wbuf.at[1 - d, p], crecv.at[p]).wait()
        return wbuf[0, p].reshape(256, D), wbuf[1, p].reshape(256, D)

    def shared_piece(p):
        up, down = shared_weights(p)

        @pl.loop(0, 4)
        def _(b):
            shared_block(p, b, up, down)

    serve(0)
    y_arrived(1)
    serve(1)
    with jax.named_scope("quadwait"):
        bytes_of(tokq.at[pl.ds(1, 2)], trecv.at[0]).wait()
        passed_on.start()
    y_arrived(2)
    serve(2)
    passed_on.wait_recv()
    shared_piece(0)
    serve(3)
    shared_piece(1)
    shared_piece(3)
    up, down = shared_weights(2)
    halves = [remote(sacc.at[1 + 2 * k], precv.at[k], psend, precv_sem.at[k], partner) for k in range(2)]
    result = remote(xsend, xrecv, osend, orecv, across)
    shared_block(2, 3, up, down)
    halves[1].start()
    shared_block(2, 1, up, down)
    halves[0].start()
    shared_block(2, 2, up, down)
    with jax.named_scope("h1wait"):
        halves[1].wait_recv()
    xsend[...] = (sacc[2] + precv[1]).astype(BF)
    result.start()
    shared_block(2, 0, up, down)
    with jax.named_scope("h0wait"):
        halves[0].wait_recv()
    rows_o[2] = (sacc[0] + precv[0]).astype(BF)

    def gather(q):
        first = 1 if q == SELF // PER else 0
        with jax.named_scope("rwait"):
            bytes_of(back.at[pl.ds(q * PER + first, PER - first)], rrecv.at[q]).wait()
        rows = flat_rows(back[pl.ds(q * PER, PER)])
        at = lax.broadcasted_iota(I32, (TOK, TOK), 1) + q * TOK
        for k in range(2):
            part = dot((at == slot_col[k]).astype(F32).astype(BF), rows)
            if q == 0:
                pacc[k] = part
            elif q < CH - 1:
                pacc[k] = pacc[k] + part
            else:
                rows_o[k] = (pacc[k] + part).astype(BF)

    for q in range(CH - 1):
        gather(q)
    with jax.named_scope("lwait"):
        bytes_of(lback.at[pl.ds(1, NEP - 1)], lrecv).wait()

    scores = lback[...].reshape(NEP, 128).astype(BF)
    lane = lax.broadcasted_iota(I32, (TOK, 128), 1)
    down_i = lax.broadcasted_iota(I32, (128, 128), 0)
    over_i = lax.broadcasted_iota(I32, (128, 128), 1)
    logits = slog[...]
    keep = jnp.ones((TOK, 128), F32)
    for k in range(2):
        col = slot_col[k]
        kept = col >= 0
        spot = jnp.where(kept, col // 8, -1)
        mine = dot((lane == spot).astype(F32).astype(BF), scores)
        mine = jnp.where(lane // 16 == jnp.where(kept, col % 8, -1), mine, 0.0).astype(BF)
        spread = jnp.logical_and(down_i % 16 == over_i % 16, (over_i // 16) % 4 == k)
        logits = logits + dot(mine, spread.astype(F32).astype(BF))
        keep = jnp.where((lane // 16) % 4 == k, kept.astype(F32), keep)
    values = keep * jax.nn.sigmoid(logits)
    pair = values + pltpu.roll(values, 16, 1)
    weights = values / (pair + pltpu.roll(pair, 32, 1))
    wide = 4 * TB
    col = lax.broadcasted_iota(I32, (128, TASKS * wide), 1)
    line = lax.broadcasted_iota(I32, (128, TASKS * wide), 0)
    take = (line == (col % wide) // TB * 16 + col // wide).astype(F32).astype(BF)
    diagonal = (
        lax.broadcasted_iota(I32, (TOK, wide), 1) % TB == lax.broadcasted_iota(I32, (TOK, wide), 0) % TB
    )
    spread = dot(weights.astype(BF), take)
    for s in range(TASKS):
        w_o[s] = jnp.where(diagonal, spread[:, s * wide : (s + 1) * wide], 0.0).astype(BF)

    with jax.named_scope("owait"):
        result.wait()
    rows_o[3] = xrecv[...]
    gather(CH - 1)
    with jax.named_scope("sendwait"):
        bytes_of(wbuf.at[0, 0, pl.ds(1, 7)], zsend).wait()
        bytes_of(wbuf.at[0, pl.ds(1, 3)], ysend).wait()
        bytes_of(wbuf.at[0], csend).wait()
        bytes_of(tokq.at[pl.ds(1, 3)], tsend).wait()
        bytes_of(precv, psend).wait()
        bytes_of(snd.at[pl.ds(1, NEP - 1)], dsend).wait()
        bytes_of(lret.at[pl.ds(1, NEP - 1)], lsend).wait()
        bytes_of(ret.at[pl.ds(1, NEP - 1)], rsend).wait()


OUT_PARTS = 8


def mix(rows_r, w_r, out_h, buf, sem):
    size = TOK // OUT_PARTS

    def put(h):
        at = pl.ds(h * size, size)
        return pltpu.make_async_copy(buf.at[:, at], out_h.at[:, at], sem.at[h])

    for b in range(TOK // TB):
        at = slice(b * TB, (b + 1) * TB)
        terms = jnp.concatenate([rows_r[i, at] for i in range(4)], axis=0)
        left = jnp.concatenate([w_r[s, at] for s in range(TASKS)], axis=0)
        made = dot(left, terms).astype(BF)
        for s in range(TASKS):
            buf[s, at] = made[s * TB : (s + 1) * TB]
        if (b + 1) * TB % size == 0:
            put((b + 1) * TB // size - 1).start()
    for h in range(OUT_PARTS):
        put(h).wait()


def on_device(tokens, routes, capacity, expert_in, expert_out, shared_in, shared_out, route_gate, shared_gate):
    hbm = pl.BlockSpec(memory_space=pltpu.HBM)
    vmem = pl.BlockSpec(memory_space=pltpu.VMEM)
    dma = pltpu.SemaphoreType.DMA
    rows, weights = pl.pallas_call(
        exchange,
        out_shape=(
            jax.ShapeDtypeStruct((4, TOK, D), BF),
            jax.ShapeDtypeStruct((TASKS, TOK, 4 * TB), BF),
        ),
        in_specs=[hbm] * 9,
        out_specs=(vmem, vmem),
        scratch_shapes=[
            pltpu.VMEM((2, TOK), I32),
            pltpu.VMEM((1, NEP), I32),
            pltpu.VMEM((1, TASKS * D), BF),
            pltpu.VMEM((2, TASKS * D), BF),
            pltpu.VMEM((D, H), BF),
            pltpu.VMEM((H, D), BF),
            pltpu.VMEM((2, 2, 16, D), BF),
            pltpu.VMEM((2, 4, 8, 2, 16, D), BF),
            pltpu.VMEM((4, TOK, D), BF),
            pltpu.VMEM((NEP, 8, D), BF),
            pltpu.VMEM((NEP, 8, D), BF),
            pltpu.VMEM((NEP, 8, D), BF),
            pltpu.VMEM((NEP, 8, D), BF),
            pltpu.VMEM((NEP, 1, 128), F32),
            pltpu.VMEM((NEP, 1, 128), F32),
            pltpu.VMEM((4, TOK, D), F32),
            pltpu.VMEM((2, TOK, D), F32),
            pltpu.VMEM((TOK, D), BF),
            pltpu.VMEM((TOK, D), BF),
            pltpu.VMEM((2, TOK, D), F32),
            pltpu.VMEM((TOK, 128), F32),
            dma((6,)),
            dma((2,)),
            dma, dma((CH,)),
            dma, dma((CH,)),
            dma, dma,
            dma, dma((2,)),
            dma, dma,
            dma, dma((2,)),
            dma, dma((3,)),
            dma, dma((2,)),
            dma, dma,
            dma, dma((4,)),
        ],
        compiler_params=pltpu.CompilerParams(collective_id=0, has_side_effects=True, vmem_limit_bytes=40 * 2**20),
        name="exchange",
    )(*[
        pltpu.with_memory_space_constraint(a, pltpu.HBM)
        for a in (
            tokens, routes.T, capacity.reshape(1, NEP), expert_in, expert_out,
            shared_in, shared_out, route_gate, shared_gate,
        )
    ])
    mixed = pl.pallas_call(
        mix,
        out_shape=jax.ShapeDtypeStruct((TASKS, TOK, D), BF),
        in_specs=[vmem, vmem],
        out_specs=hbm,
        scratch_shapes=[pltpu.VMEM((TASKS, TOK, D), BF), dma((OUT_PARTS,))],
        compiler_params=pltpu.CompilerParams(vmem_limit_bytes=24 * 2**20),
        name="mix",
    )(rows, weights)
    return mixed.transpose(1, 0, 2)


def solution(mesh):
    rows, experts = P(("dp", "ep"), None), P("ep", None, None)
    return jax.shard_map(
        on_device,
        mesh=mesh,
        in_specs=(rows, rows, P(), experts, experts, P(None, "ep", None), P(None, "ep", None), P("ep", None), P()),
        out_specs=P(("dp", "ep"), None, None),
        check_vma=False,
    )
```

```python
import jax
import jax.numpy as jnp
from jax import lax
from jax.experimental import pallas as pl
from jax.experimental.pallas import tpu as pltpu
from jax.sharding import PartitionSpec as P

BF = jnp.bfloat16
F32 = jnp.float32
I32 = jnp.int32
MESH = pl.DeviceIdType.MESH
D = 512
H = 2048
TASKS = 12
TOK = 256
NEP = 128
CH = 4
PER = NEP // CH
SELF = 2 * PER


TB = 32
ZSTEP = (0, 1, 7, 2, 6, 3, 5, 4)
PARTS = ((0, 1), (1, 4), (5, 3))


def gelu(x):
    return jax.nn.gelu(x, approximate=True)


def dot(a, b, dims=((1,), (0,))):
    return lax.dot_general(a, b, (dims, ((), ())), preferred_element_type=F32)


def flat_rows(blocks):
    return blocks.astype(F32).reshape(-1, D).astype(BF)


def block_rows(rows):
    return rows.reshape(-1, 8, D).astype(BF)


def gate_tile(rows, group):
    sub = lax.broadcasted_iota(I32, (16, D), 0)
    tiles = []
    for row in rows:
        tile = jnp.zeros((16, D), F32)
        for s in range(TASKS):
            tile = jnp.where(sub == s, row[:, s * D : (s + 1) * D], tile)
        tiles.append(tile)
    zero = jnp.zeros((16, D), F32)
    picked = [zero if group(g) is None else tiles[group(g)] for g in range(8)]
    return jnp.concatenate(picked, axis=0).astype(BF)


def exchange(
    tok_h, routes_h, cap_h, ein_h, eout_h, sin_h, sout_h, rg_h, sg_h,
    rows_o, w_o,
    routes_v, cap_v, rg_v, sg_v, ein_v, eout_v, xs, wbuf, tokq,
    snd, recv, ret, back, lret, lback, sacc, precv, xsend, xrecv, pacc, slog,
    load_sem, big_sem, dsend, drecv, rsend, rrecv, lsend, lrecv,
    tsend, trecv, xssem, xrsem, zsend, zrecv, ysend, yrecv, psend, precv_sem, osend, orecv, csend, crecv,
):
    me = lax.axis_index("ep")
    x, z, y, c = me >> 6, (me >> 3) & 7, (me >> 1) & 3, me & 1
    d = lax.axis_index("dp")
    mine = x ^ d
    xpart = [x * 64, (1 - x) * 64]
    zpart = [((z + d) & 7) * 8 for d in range(8)]
    cpart = [c, 1 - c]

    def load(src, dst, k):
        return pltpu.make_async_copy(src, dst, load_sem.at[k])

    loads = [
        load(routes_h, routes_v, 0),
        load(cap_h, cap_v, 1),
        load(tok_h, tokq.at[0], 2),
        load(rg_h, rg_v, 3),
        load(sg_h, sg_v, 4),
    ]
    for k in loads:
        k.start()
    load(sin_h, xs.at[0], 5).start()
    load(sout_h, xs.at[1], 5).start()
    big = [
        pltpu.make_async_copy(ein_h.at[0], ein_v, big_sem.at[0]),
        pltpu.make_async_copy(eout_h.at[0], eout_v, big_sem.at[1]),
    ]
    for k in big:
        k.start()

    barrier = pltpu.get_barrier_semaphore()
    other = {"dp": 1 - d, "ep": xpart[1] + (me & 63)}
    pl.semaphore_signal(barrier, inc=1, device_id=other, device_id_type=MESH)
    for dz in (4, 3, 5, 2, 6, 1, 7, 0):
        for dy in (2, 1, 3, 0):
            for dx in (1, 0):
                for dc in (1, 0):
                    if dz or dy or dx or dc:
                        to = xpart[dx] + zpart[dz] + ((y + dy) & 3) * 2 + cpart[dc]
                        pl.semaphore_signal(barrier, inc=1, device_id={"ep": to}, device_id_type=MESH)

    with jax.named_scope("loadwait"):
        for k in loads:
            k.wait()
        load(xs, xs, 5).wait()

    expert = lax.broadcasted_iota(I32, (NEP, 1), 0)
    dz = ((expert >> 3) - z + 8) & 7
    zi = jnp.where(dz == 0, 0, jnp.where(dz <= 4, 2 * dz - 1, 2 * (8 - dz)))
    place = (((((expert - c + 2) & 1) + 2 - 2 * (((expert >> 6) - x + 2) & 1)) * 4) + (((expert >> 1) - y + 4) & 3)) * 8 + zi
    base = (place * 8).astype(F32)
    named = lax.broadcasted_iota(I32, (NEP, TOK), 0)
    chosen = [(named == routes_v[k : k + 1, :]).astype(F32) for k in range(2)]
    earlier = (
        lax.broadcasted_iota(I32, (TOK, TOK), 0) < lax.broadcasted_iota(I32, (TOK, TOK), 1)
    ).astype(BF)
    before = dot((chosen[0] + chosen[1]).astype(BF), earlier)
    cap = jnp.broadcast_to(cap_v[...].astype(F32), (8, NEP)).astype(BF)
    slots = []
    for k in range(2):
        rank = jnp.sum(chosen[k] * before, axis=0, keepdims=True)
        start = jnp.sum(chosen[k] * base, axis=0, keepdims=True)
        limit = dot(cap, chosen[k].astype(BF))[0:1]
        slots.append(jnp.where(rank < limit, start + rank, -1.0))
    slot_row = [s.astype(I32) for s in slots]
    slot_col = [
        jnp.transpose(jnp.broadcast_to(s, (128, TOK)))[:, 0:1].astype(I32) for s in slots
    ]

    own = tokq[0]
    for q in range(CH):
        at = lax.broadcasted_iota(I32, (TOK, TOK), 0) + q * TOK
        pick = jnp.logical_or(at == slot_row[0], at == slot_row[1]).astype(F32).astype(BF)
        rows = block_rows(dot(pick, own))
        snd[pl.ds(q * PER, PER)] = rows
        if q == SELF // PER:
            recv[SELF : SELF + 1] = rows[0:1]

    wbuf[d, 0, 0, x] = xs[d, mine]
    gates = gate_tile([rg_v[...].astype(F32)], lambda g: 0)
    sg = sg_v[...].astype(F32)
    sg_own = jnp.where(mine == 0, sg[0:1], sg[1:2])
    sg_other = jnp.where(mine == 0, sg[1:2], sg[0:1])
    shared_gates = gate_tile([sg_own, sg_other], lambda g: g % 4 - 2 if g % 4 >= 2 else None)
    slog[...] = dot(own, shared_gates, ((1,), (1,))).astype(BF).astype(F32)

    with jax.named_scope("barrier"):
        pl.semaphore_wait(barrier, NEP)

    def remote(src, dst, ss, rs, to):
        return pltpu.make_async_remote_copy(
            src_ref=src, dst_ref=dst, send_sem=ss, recv_sem=rs,
            device_id=to if isinstance(to, dict) else {"ep": to}, device_id_type=MESH,
        )

    def bytes_of(a, sem):
        return pltpu.make_async_copy(a, a, sem)

    def toward(dx, dz, dy, dc):
        return xpart[dx] + zpart[dz] + ((y + dy) & 3) * 2 + cpart[dc]

    def each(q, low, high, sign, act):
        dx, dc = 1 - q // 2, q % 2
        if q == SELF // PER and low == 0:
            for i in range(1, 8):
                act(SELF + i, toward(dx, sign * ZSTEP[i] % 8, 0, dc))
            low = 1

        @pl.loop(low, high)
        def _(dy):
            for i in range(8):
                act(q * PER + dy * 8 + i, toward(dx, sign * ZSTEP[i] % 8, 4 + sign * dy, dc))

    across = toward(1, 0, 0, 0)
    partner = toward(0, 0, 0, 1)

    def dispatch(q, low=0, high=4):
        each(q, low, high, 1, lambda n, to: remote(snd.at[n], recv.at[n], dsend, drecv.at[q], to).start())

    x_half = remote(xs.at[d, 1 - mine], wbuf.at[d, 0, 0, x], xssem, xrsem, across)
    x_half.start()
    dispatch(0, 0, 2)
    with jax.named_scope("xwait"):
        x_half.wait()

    def along_z(src, slot, k, dz):
        return remote(src, wbuf.at[(d, 0) + slot], zsend, zrecv.at[k], toward(0, dz, 0, 0))

    near = [along_z(wbuf.at[d, 0, 0], (1,), 0, 1), along_z(wbuf.at[d, 0, 0], (2,), 0, 7)]
    next_near = [along_z(wbuf.at[d, 0, 1], (3,), 2, 1), along_z(wbuf.at[d, 0, 2], (4,), 2, 7)]
    far = [
        along_z(wbuf.at[d, 0, 3], (5,), 1, 1),
        along_z(wbuf.at[d, 0, 4], (6,), 1, 7),
        along_z(wbuf.at[d, 0, 3, 0], (7, 0), 1, 2),
        along_z(wbuf.at[d, 0, 4, 1], (7, 1), 1, 6),
    ]
    along_y = []
    for j, (first, count) in enumerate(PARTS):
        along_y.append({
            dy: remote(
                wbuf.at[d, 0, pl.ds(first, count)], wbuf.at[d, dy, pl.ds(first, count)],
                ysend, yrecv.at[j], toward(0, 0, dy, 0),
            )
            for dy in (1, 3, 2)
        })
    swap = []
    for j, (first, count) in enumerate(PARTS):
        swap.append([
            remote(
                wbuf.at[d, p, pl.ds(first, count)], wbuf.at[d, p, pl.ds(first, count)],
                csend, crecv.at[p], other,
            )
            for p in range(4)
        ])
    quad = [
        remote(tokq.at[0], tokq.at[p], tsend, trecv.at[0], to)
        for p, to in ((1, partner), (2, across))
    ]
    passed_on = remote(tokq.at[2], tokq.at[3], tsend, trecv.at[1], partner)

    def y_arrived(j):
        with jax.named_scope("ywait"):
            first, count = PARTS[j]
            bytes_of(wbuf.at[d, pl.ds(1, 3), pl.ds(first, count)], yrecv.at[j]).wait()
        for dy in (1, 3, 2):
            swap[j][dy].start()

    for k in near:
        k.start()
    for k in along_y[0].values():
        k.start()
    swap[0][0].start()
    dispatch(0, 2, 4)
    dispatch(1, 0, 2)
    with jax.named_scope("nearwait"):
        bytes_of(wbuf.at[d, 0, pl.ds(1, 2)], zrecv.at[0]).wait()
    for k in next_near:
        k.start()
    dispatch(1, 2, 4)
    dispatch(2, 0, 2)
    for k in quad:
        k.start()
    with jax.named_scope("nextwait"):
        bytes_of(wbuf.at[d, 0, pl.ds(3, 2)], zrecv.at[2]).wait()
    for k in far:
        k.start()
    for k in along_y[1].values():
        k.start()
    swap[1][0].start()
    dispatch(2, 2, 4)
    dispatch(3)
    y_arrived(0)
    for k in big:
        k.wait()

    fold = (
        lax.broadcasted_iota(I32, (TOK, 128), 1) // 16 == lax.broadcasted_iota(I32, (TOK, 128), 0) % 8
    )

    def serve(q):
        first = 1 if q == SELF // PER else 0
        with jax.named_scope("dwait"):
            bytes_of(recv.at[pl.ds(q * PER + first, PER - first)], drecv.at[q]).wait()
        rows = flat_rows(recv[pl.ds(q * PER, PER)])
        scores = dot(rows, gates, ((1,), (1,))).astype(BF).astype(F32)
        scores = jnp.sum(
            jnp.where(fold, scores, 0.0).reshape(PER, 8, 128), axis=1, keepdims=True
        )
        lret[pl.ds(q * PER, PER)] = scores
        if q == SELF // PER:
            lback[SELF : SELF + 1] = scores[0:1]
        total = jnp.zeros((TOK, D), F32)
        for t in range(4):
            hidden = gelu(dot(rows, ein_v[:, t * 512 : (t + 1) * 512])).astype(BF)
            total = total + dot(hidden, eout_v[t * 512 : (t + 1) * 512, :])
        made = block_rows(total)
        ret[pl.ds(q * PER, PER)] = made
        if q == SELF // PER:
            back[SELF : SELF + 1] = made[0:1]
        with jax.named_scope("logsend"):
            each(q, 0, 4, -1, lambda n, to: remote(lret.at[n], lback.at[n], lsend, lrecv, to).start())
        with jax.named_scope("retsend"):
            if q < CH - 1:
                each(q, 0, 4, -1, lambda n, to: remote(ret.at[n], back.at[n], rsend, rrecv.at[q], to).start())
            else:
                for i in (7, 6, 5, 4, 3, 2, 1, 0):
                    for dy in (2, 1, 3, 0):
                        n = q * PER + dy * 8 + i
                        to = toward(1 - q // 2, -ZSTEP[i] % 8, 4 - dy, q % 2)
                        remote(ret.at[n], back.at[n], rsend, rrecv.at[q], to).start()

    def shared_block(p, b, up, down):
        hidden = gelu(dot(tokq[b], up, ((1,), (1,)))).astype(BF)
        part = dot(hidden, down)
        if p == 0:
            sacc[b] = part
        else:
            sacc[b] = sacc[b] + part

    def shared_weights(p):
        with jax.named_scope("swapwait"):
            bytes_of(wbuf.at[1 - d, p], crecv.at[p]).wait()
        return wbuf[0, p].reshape(256, D), wbuf[1, p].reshape(256, D)

    def shared_piece(p):
        up, down = shared_weights(p)

        @pl.loop(0, 4)
        def _(b):
            shared_block(p, b, up, down)

    serve(0)
    with jax.named_scope("farwait"):
        bytes_of(wbuf.at[d, 0, pl.ds(5, 3)], zrecv.at[1]).wait()
    for k in along_y[2].values():
        k.start()
    swap[2][0].start()
    y_arrived(1)
    serve(1)
    with jax.named_scope("quadwait"):
        bytes_of(tokq.at[pl.ds(1, 2)], trecv.at[0]).wait()
        passed_on.start()
    y_arrived(2)
    serve(2)
    passed_on.wait_recv()
    shared_piece(0)
    serve(3)
    shared_piece(1)
    shared_piece(3)
    up, down = shared_weights(2)
    halves = [remote(sacc.at[1 + 2 * k], precv.at[k], psend, precv_sem.at[k], partner) for k in range(2)]
    result = remote(xsend, xrecv, osend, orecv, across)
    shared_block(2, 3, up, down)
    halves[1].start()
    shared_block(2, 1, up, down)
    halves[0].start()
    shared_block(2, 2, up, down)
    with jax.named_scope("h1wait"):
        halves[1].wait_recv()
    xsend[...] = (sacc[2] + precv[1]).astype(BF)
    result.start()
    shared_block(2, 0, up, down)
    with jax.named_scope("h0wait"):
        halves[0].wait_recv()
    rows_o[2] = (sacc[0] + precv[0]).astype(BF)

    def gather(q):
        first = 1 if q == SELF // PER else 0
        with jax.named_scope("rwait"):
            bytes_of(back.at[pl.ds(q * PER + first, PER - first)], rrecv.at[q]).wait()
        rows = flat_rows(back[pl.ds(q * PER, PER)])
        at = lax.broadcasted_iota(I32, (TOK, TOK), 1) + q * TOK
        for k in range(2):
            part = dot((at == slot_col[k]).astype(F32).astype(BF), rows)
            if q == 0:
                pacc[k] = part
            elif q < CH - 1:
                pacc[k] = pacc[k] + part
            else:
                rows_o[k] = (pacc[k] + part).astype(BF)

    for q in range(CH - 1):
        gather(q)
    with jax.named_scope("lwait"):
        bytes_of(lback.at[pl.ds(1, NEP - 1)], lrecv).wait()

    scores = lback[...].reshape(NEP, 128).astype(BF)
    lane = lax.broadcasted_iota(I32, (TOK, 128), 1)
    down_i = lax.broadcasted_iota(I32, (128, 128), 0)
    over_i = lax.broadcasted_iota(I32, (128, 128), 1)
    logits = slog[...]
    keep = jnp.ones((TOK, 128), F32)
    for k in range(2):
        col = slot_col[k]
        kept = col >= 0
        spot = jnp.where(kept, col // 8, -1)
        mine = dot((lane == spot).astype(F32).astype(BF), scores)
        mine = jnp.where(lane // 16 == jnp.where(kept, col % 8, -1), mine, 0.0).astype(BF)
        spread = jnp.logical_and(down_i % 16 == over_i % 16, (over_i // 16) % 4 == k)
        logits = logits + dot(mine, spread.astype(F32).astype(BF))
        keep = jnp.where((lane // 16) % 4 == k, kept.astype(F32), keep)
    values = keep * jax.nn.sigmoid(logits)
    pair = values + pltpu.roll(values, 16, 1)
    weights = values / (pair + pltpu.roll(pair, 32, 1))
    wide = 4 * TB
    col = lax.broadcasted_iota(I32, (128, TASKS * wide), 1)
    line = lax.broadcasted_iota(I32, (128, TASKS * wide), 0)
    take = (line == (col % wide) // TB * 16 + col // wide).astype(F32).astype(BF)
    diagonal = (
        lax.broadcasted_iota(I32, (TOK, wide), 1) % TB == lax.broadcasted_iota(I32, (TOK, wide), 0) % TB
    )
    spread = dot(weights.astype(BF), take)
    for s in range(TASKS):
        w_o[s] = jnp.where(diagonal, spread[:, s * wide : (s + 1) * wide], 0.0).astype(BF)

    with jax.named_scope("owait"):
        result.wait()
    rows_o[3] = xrecv[...]
    gather(CH - 1)
    with jax.named_scope("sendwait"):
        bytes_of(wbuf.at[0, 0, pl.ds(1, 7)], zsend).wait()
        bytes_of(wbuf.at[0, pl.ds(1, 3)], ysend).wait()
        bytes_of(wbuf.at[0], csend).wait()
        bytes_of(tokq.at[pl.ds(1, 3)], tsend).wait()
        bytes_of(precv, psend).wait()
        bytes_of(snd.at[pl.ds(1, NEP - 1)], dsend).wait()
        bytes_of(lret.at[pl.ds(1, NEP - 1)], lsend).wait()
        bytes_of(ret.at[pl.ds(1, NEP - 1)], rsend).wait()


OUT_PARTS = 8


def mix(rows_r, w_r, out_h, buf, sem):
    size = TOK // OUT_PARTS

    def put(h):
        at = pl.ds(h * size, size)
        return pltpu.make_async_copy(buf.at[:, at], out_h.at[:, at], sem.at[h])

    for b in range(TOK // TB):
        at = slice(b * TB, (b + 1) * TB)
        terms = jnp.concatenate([rows_r[i, at] for i in range(4)], axis=0)
        left = jnp.concatenate([w_r[s, at] for s in range(TASKS)], axis=0)
        made = dot(left, terms).astype(BF)
        for s in range(TASKS):
            buf[s, at] = made[s * TB : (s + 1) * TB]
        if (b + 1) * TB % size == 0:
            put((b + 1) * TB // size - 1).start()
    for h in range(OUT_PARTS):
        put(h).wait()


def on_device(tokens, routes, capacity, expert_in, expert_out, shared_in, shared_out, route_gate, shared_gate):
    hbm = pl.BlockSpec(memory_space=pltpu.HBM)
    vmem = pl.BlockSpec(memory_space=pltpu.VMEM)
    dma = pltpu.SemaphoreType.DMA
    rows, weights = pl.pallas_call(
        exchange,
        out_shape=(
            jax.ShapeDtypeStruct((4, TOK, D), BF),
            jax.ShapeDtypeStruct((TASKS, TOK, 4 * TB), BF),
        ),
        in_specs=[hbm] * 9,
        out_specs=(vmem, vmem),
        scratch_shapes=[
            pltpu.VMEM((2, TOK), I32),
            pltpu.VMEM((1, NEP), I32),
            pltpu.VMEM((1, TASKS * D), BF),
            pltpu.VMEM((2, TASKS * D), BF),
            pltpu.VMEM((D, H), BF),
            pltpu.VMEM((H, D), BF),
            pltpu.VMEM((2, 2, 16, D), BF),
            pltpu.VMEM((2, 4, 8, 2, 16, D), BF),
            pltpu.VMEM((4, TOK, D), BF),
            pltpu.VMEM((NEP, 8, D), BF),
            pltpu.VMEM((NEP, 8, D), BF),
            pltpu.VMEM((NEP, 8, D), BF),
            pltpu.VMEM((NEP, 8, D), BF),
            pltpu.VMEM((NEP, 1, 128), F32),
            pltpu.VMEM((NEP, 1, 128), F32),
            pltpu.VMEM((4, TOK, D), F32),
            pltpu.VMEM((2, TOK, D), F32),
            pltpu.VMEM((TOK, D), BF),
            pltpu.VMEM((TOK, D), BF),
            pltpu.VMEM((2, TOK, D), F32),
            pltpu.VMEM((TOK, 128), F32),
            dma((6,)),
            dma((2,)),
            dma, dma((CH,)),
            dma, dma((CH,)),
            dma, dma,
            dma, dma((2,)),
            dma, dma,
            dma, dma((3,)),
            dma, dma((3,)),
            dma, dma((2,)),
            dma, dma,
            dma, dma((4,)),
        ],
        compiler_params=pltpu.CompilerParams(collective_id=0, has_side_effects=True, vmem_limit_bytes=40 * 2**20),
        name="exchange",
    )(*[
        pltpu.with_memory_space_constraint(a, pltpu.HBM)
        for a in (
            tokens, routes.T, capacity.reshape(1, NEP), expert_in, expert_out,
            shared_in, shared_out, route_gate, shared_gate,
        )
    ])
    mixed = pl.pallas_call(
        mix,
        out_shape=jax.ShapeDtypeStruct((TASKS, TOK, D), BF),
        in_specs=[vmem, vmem],
        out_specs=hbm,
        scratch_shapes=[pltpu.VMEM((TASKS, TOK, D), BF), dma((OUT_PARTS,))],
        compiler_params=pltpu.CompilerParams(vmem_limit_bytes=24 * 2**20),
        name="mix",
    )(rows, weights)
    return mixed.transpose(1, 0, 2)


def solution(mesh):
    rows, experts = P(("dp", "ep"), None), P("ep", None, None)
    return jax.shard_map(
        on_device,
        mesh=mesh,
        in_specs=(rows, rows, P(), experts, experts, P(None, "ep", None), P(None, "ep", None), P("ep", None), P()),
        out_specs=P(("dp", "ep"), None, None),
        check_vma=False,
    )
```

```python
import jax
import jax.numpy as jnp
from jax import lax
from jax.experimental import pallas as pl
from jax.experimental.pallas import tpu as pltpu
from jax.sharding import PartitionSpec as P

BF = jnp.bfloat16
F32 = jnp.float32
I32 = jnp.int32
MESH = pl.DeviceIdType.MESH
D = 512
H = 2048
TASKS = 12
TOK = 256
NEP = 128
CH = 4
PER = NEP // CH
SELF = 2 * PER


TB = 32
ZSTEP = (0, 1, 7, 2, 6, 3, 5, 4)
PARTS = ((0, 1), (1, 4), (5, 3))


def gelu(x):
    return jax.nn.gelu(x, approximate=True)


def dot(a, b, dims=((1,), (0,))):
    return lax.dot_general(a, b, (dims, ((), ())), preferred_element_type=F32)


def flat_rows(blocks):
    return blocks.astype(F32).reshape(-1, D).astype(BF)


def block_rows(rows):
    return rows.reshape(-1, 8, D).astype(BF)


def gate_tile(rows, group):
    sub = lax.broadcasted_iota(I32, (16, D), 0)
    tiles = []
    for row in rows:
        tile = jnp.zeros((16, D), F32)
        for s in range(TASKS):
            tile = jnp.where(sub == s, row[:, s * D : (s + 1) * D], tile)
        tiles.append(tile)
    zero = jnp.zeros((16, D), F32)
    picked = [zero if group(g) is None else tiles[group(g)] for g in range(8)]
    return jnp.concatenate(picked, axis=0).astype(BF)


def exchange(
    tok_h, routes_h, cap_h, ein_h, eout_h, sin_h, sout_h, rg_h, sg_h,
    rows_o, w_o,
    routes_v, cap_v, rg_v, sg_v, ein_v, eout_v, xs, wbuf, tokq,
    snd, recv, ret, back, lret, lback, sacc, precv, xsend, xrecv, pacc, slog,
    load_sem, big_sem, dsend, drecv, rsend, rrecv, lsend, lrecv,
    tsend, trecv, xssem, xrsem, zsend, zrecv, ysend, yrecv, psend, precv_sem, osend, orecv, csend, crecv,
):
    me = lax.axis_index("ep")
    x, z, y, c = me >> 6, (me >> 3) & 7, (me >> 1) & 3, me & 1
    d = lax.axis_index("dp")
    mine = x ^ d
    xpart = [x * 64, (1 - x) * 64]
    zpart = [((z + d) & 7) * 8 for d in range(8)]
    cpart = [c, 1 - c]

    def load(src, dst, k):
        return pltpu.make_async_copy(src, dst, load_sem.at[k])

    loads = [
        load(routes_h, routes_v, 0),
        load(cap_h, cap_v, 1),
        load(tok_h, tokq.at[0], 2),
        load(rg_h, rg_v, 3),
        load(sg_h, sg_v, 4),
    ]
    for k in loads:
        k.start()
    load(sin_h, xs.at[0], 5).start()
    load(sout_h, xs.at[1], 5).start()
    big = [
        pltpu.make_async_copy(ein_h.at[0], ein_v, big_sem.at[0]),
        pltpu.make_async_copy(eout_h.at[0], eout_v, big_sem.at[1]),
    ]
    for k in big:
        k.start()

    barrier = pltpu.get_barrier_semaphore()
    other = {"dp": 1 - d, "ep": xpart[1] + (me & 63)}
    pl.semaphore_signal(barrier, inc=1, device_id=other, device_id_type=MESH)
    for dz in (4, 3, 5, 2, 6, 1, 7, 0):
        for dy in (2, 1, 3, 0):
            for dx in (1, 0):
                for dc in (1, 0):
                    if dz or dy or dx or dc:
                        to = xpart[dx] + zpart[dz] + ((y + dy) & 3) * 2 + cpart[dc]
                        pl.semaphore_signal(barrier, inc=1, device_id={"ep": to}, device_id_type=MESH)

    with jax.named_scope("loadwait"):
        for k in loads:
            k.wait()
        load(xs, xs, 5).wait()

    expert = lax.broadcasted_iota(I32, (NEP, 1), 0)
    dz = ((expert >> 3) - z + 8) & 7
    zi = jnp.where(dz == 0, 0, jnp.where(dz <= 4, 2 * dz - 1, 2 * (8 - dz)))
    place = (((((expert - c + 2) & 1) + 2 - 2 * (((expert >> 6) - x + 2) & 1)) * 4) + (((expert >> 1) - y + 4) & 3)) * 8 + zi
    base = (place * 8).astype(F32)
    named = lax.broadcasted_iota(I32, (NEP, TOK), 0)
    chosen = [(named == routes_v[k : k + 1, :]).astype(F32) for k in range(2)]
    earlier = (
        lax.broadcasted_iota(I32, (TOK, TOK), 0) < lax.broadcasted_iota(I32, (TOK, TOK), 1)
    ).astype(BF)
    before = dot((chosen[0] + chosen[1]).astype(BF), earlier)
    cap = jnp.broadcast_to(cap_v[...].astype(F32), (8, NEP)).astype(BF)
    slots = []
    for k in range(2):
        rank = jnp.sum(chosen[k] * before, axis=0, keepdims=True)
        start = jnp.sum(chosen[k] * base, axis=0, keepdims=True)
        limit = dot(cap, chosen[k].astype(BF))[0:1]
        slots.append(jnp.where(rank < limit, start + rank, -1.0))
    slot_row = [s.astype(I32) for s in slots]
    slot_col = [
        jnp.transpose(jnp.broadcast_to(s, (128, TOK)))[:, 0:1].astype(I32) for s in slots
    ]

    own = tokq[0]
    for q in range(CH):
        at = lax.broadcasted_iota(I32, (TOK, TOK), 0) + q * TOK
        pick = jnp.logical_or(at == slot_row[0], at == slot_row[1]).astype(F32).astype(BF)
        rows = block_rows(dot(pick, own))
        snd[pl.ds(q * PER, PER)] = rows
        if q == SELF // PER:
            recv[SELF : SELF + 1] = rows[0:1]

    wbuf[d, 0, 0, x] = xs[d, mine]
    gates = gate_tile([rg_v[...].astype(F32)], lambda g: 0)
    sg = sg_v[...].astype(F32)
    sg_own = jnp.where(mine == 0, sg[0:1], sg[1:2])
    sg_other = jnp.where(mine == 0, sg[1:2], sg[0:1])
    shared_gates = gate_tile([sg_own, sg_other], lambda g: g % 4 - 2 if g % 4 >= 2 else None)
    slog[...] = dot(own, shared_gates, ((1,), (1,))).astype(BF).astype(F32)

    with jax.named_scope("barrier"):
        pl.semaphore_wait(barrier, NEP)

    def remote(src, dst, ss, rs, to):
        return pltpu.make_async_remote_copy(
            src_ref=src, dst_ref=dst, send_sem=ss, recv_sem=rs,
            device_id=to if isinstance(to, dict) else {"ep": to}, device_id_type=MESH,
        )

    def bytes_of(a, sem):
        return pltpu.make_async_copy(a, a, sem)

    def toward(dx, dz, dy, dc):
        return xpart[dx] + zpart[dz] + ((y + dy) & 3) * 2 + cpart[dc]

    def each(q, low, high, sign, act):
        dx, dc = 1 - q // 2, q % 2
        if q == SELF // PER and low == 0:
            for i in range(1, 8):
                act(SELF + i, toward(dx, sign * ZSTEP[i] % 8, 0, dc))
            low = 1

        @pl.loop(low, high)
        def _(dy):
            for i in range(8):
                act(q * PER + dy * 8 + i, toward(dx, sign * ZSTEP[i] % 8, 4 + sign * dy, dc))

    across = toward(1, 0, 0, 0)
    partner = toward(0, 0, 0, 1)

    def dispatch(q, low=0, high=4):
        each(q, low, high, 1, lambda n, to: remote(snd.at[n], recv.at[n], dsend, drecv.at[q], to).start())

    x_half = remote(xs.at[d, 1 - mine], wbuf.at[d, 0, 0, x], xssem, xrsem, across)
    x_half.start()
    dispatch(0, 0, 2)
    with jax.named_scope("xwait"):
        x_half.wait()

    def along_z(src, slot, k, dz):
        return remote(src, wbuf.at[(d, 0) + slot], zsend, zrecv.at[k], toward(0, dz, 0, 0))

    near = [along_z(wbuf.at[d, 0, 0], (1,), 0, 1), along_z(wbuf.at[d, 0, 0], (2,), 0, 7)]
    next_near = [along_z(wbuf.at[d, 0, 1], (3,), 2, 1), along_z(wbuf.at[d, 0, 2], (4,), 2, 7)]
    far = [
        along_z(wbuf.at[d, 0, 3], (5,), 1, 1),
        along_z(wbuf.at[d, 0, 4], (6,), 1, 7),
        along_z(wbuf.at[d, 0, 3, 0], (7, 0), 1, 2),
        along_z(wbuf.at[d, 0, 4, 1], (7, 1), 1, 6),
    ]
    along_y = []
    for j, (first, count) in enumerate(PARTS):
        along_y.append({
            dy: remote(
                wbuf.at[d, 0, pl.ds(first, count)], wbuf.at[d, dy, pl.ds(first, count)],
                ysend, yrecv.at[j], toward(0, 0, dy, 0),
            )
            for dy in (1, 3, 2)
        })
    swap = []
    for j, (first, count) in enumerate(PARTS):
        swap.append([
            remote(
                wbuf.at[d, p, pl.ds(first, count)], wbuf.at[d, p, pl.ds(first, count)],
                csend, crecv.at[p], other,
            )
            for p in range(4)
        ])
    quad = [
        remote(tokq.at[0], tokq.at[p], tsend, trecv.at[0], to)
        for p, to in ((1, partner), (2, across))
    ]
    passed_on = remote(tokq.at[2], tokq.at[3], tsend, trecv.at[1], partner)

    def y_arrived(j):
        with jax.named_scope("ywait"):
            first, count = PARTS[j]
            bytes_of(wbuf.at[d, pl.ds(1, 3), pl.ds(first, count)], yrecv.at[j]).wait()
        for dy in (1, 3, 2):
            swap[j][dy].start()

    for k in near:
        k.start()
    for k in along_y[0].values():
        k.start()
    swap[0][0].start()
    dispatch(0, 2, 4)
    dispatch(1, 0, 2)
    with jax.named_scope("nearwait"):
        bytes_of(wbuf.at[d, 0, pl.ds(1, 2)], zrecv.at[0]).wait()
    for k in next_near:
        k.start()
    dispatch(1, 2, 4)
    dispatch(2, 0, 2)
    for k in quad:
        k.start()
    with jax.named_scope("nextwait"):
        bytes_of(wbuf.at[d, 0, pl.ds(3, 2)], zrecv.at[2]).wait()
    for k in far:
        k.start()
    for k in along_y[1].values():
        k.start()
    swap[1][0].start()
    dispatch(2, 2, 4)
    dispatch(3)
    y_arrived(0)
    for k in big:
        k.wait()

    fold = (
        lax.broadcasted_iota(I32, (TOK, 128), 1) // 16 == lax.broadcasted_iota(I32, (TOK, 128), 0) % 8
    )

    def serve(q):
        first = 1 if q == SELF // PER else 0
        with jax.named_scope("dwait"):
            bytes_of(recv.at[pl.ds(q * PER + first, PER - first)], drecv.at[q]).wait()
        rows = flat_rows(recv[pl.ds(q * PER, PER)])
        scores = dot(rows, gates, ((1,), (1,))).astype(BF).astype(F32)
        scores = jnp.sum(
            jnp.where(fold, scores, 0.0).reshape(PER, 8, 128), axis=1, keepdims=True
        )
        lret[pl.ds(q * PER, PER)] = scores
        if q == SELF // PER:
            lback[SELF : SELF + 1] = scores[0:1]
        total = jnp.zeros((TOK, D), F32)
        for t in range(4):
            hidden = gelu(dot(rows, ein_v[:, t * 512 : (t + 1) * 512])).astype(BF)
            total = total + dot(hidden, eout_v[t * 512 : (t + 1) * 512, :])
        made = block_rows(total)
        ret[pl.ds(q * PER, PER)] = made
        if q == SELF // PER:
            back[SELF : SELF + 1] = made[0:1]
        with jax.named_scope("logsend"):
            if q < CH - 1:
                each(q, 0, 4, -1, lambda n, to: remote(lret.at[n], lback.at[n], lsend, lrecv, to).start())
            else:
                for i in (7, 6, 5, 4, 3, 2, 1, 0):
                    for dy in (2, 1, 3, 0):
                        n = q * PER + dy * 8 + i
                        to = toward(1 - q // 2, -ZSTEP[i] % 8, 4 - dy, q % 2)
                        remote(lret.at[n], lback.at[n], lsend, lrecv, to).start()
        with jax.named_scope("retsend"):
            if q < CH - 1:
                each(q, 0, 4, -1, lambda n, to: remote(ret.at[n], back.at[n], rsend, rrecv.at[q], to).start())
            else:
                for i in (7, 6, 5, 4, 3, 2, 1, 0):
                    for dy in (2, 1, 3, 0):
                        n = q * PER + dy * 8 + i
                        to = toward(1 - q // 2, -ZSTEP[i] % 8, 4 - dy, q % 2)
                        remote(ret.at[n], back.at[n], rsend, rrecv.at[q], to).start()

    def shared_block(p, b, up, down):
        hidden = gelu(dot(tokq[b], up, ((1,), (1,)))).astype(BF)
        part = dot(hidden, down)
        if p == 0:
            sacc[b] = part
        else:
            sacc[b] = sacc[b] + part

    def shared_weights(p):
        with jax.named_scope("swapwait"):
            bytes_of(wbuf.at[1 - d, p], crecv.at[p]).wait()
        return wbuf[0, p].reshape(256, D), wbuf[1, p].reshape(256, D)

    def shared_piece(p):
        up, down = shared_weights(p)

        @pl.loop(0, 4)
        def _(b):
            shared_block(p, b, up, down)

    serve(0)
    with jax.named_scope("farwait"):
        bytes_of(wbuf.at[d, 0, pl.ds(5, 3)], zrecv.at[1]).wait()
    for k in along_y[2].values():
        k.start()
    swap[2][0].start()
    y_arrived(1)
    serve(1)
    with jax.named_scope("quadwait"):
        bytes_of(tokq.at[pl.ds(1, 2)], trecv.at[0]).wait()
        passed_on.start()
    serve(2)
    y_arrived(2)
    passed_on.wait_recv()
    shared_piece(0)
    serve(3)
    shared_piece(1)
    shared_piece(3)
    up, down = shared_weights(2)
    halves = [remote(sacc.at[1 + 2 * k], precv.at[k], psend, precv_sem.at[k], partner) for k in range(2)]
    result = remote(xsend, xrecv, osend, orecv, across)
    shared_block(2, 3, up, down)
    halves[1].start()
    shared_block(2, 1, up, down)
    halves[0].start()
    shared_block(2, 2, up, down)
    with jax.named_scope("h1wait"):
        halves[1].wait_recv()
    xsend[...] = (sacc[2] + precv[1]).astype(BF)
    result.start()
    shared_block(2, 0, up, down)
    with jax.named_scope("h0wait"):
        halves[0].wait_recv()
    rows_o[2] = (sacc[0] + precv[0]).astype(BF)

    def gather(q):
        first = 1 if q == SELF // PER else 0
        with jax.named_scope("rwait"):
            bytes_of(back.at[pl.ds(q * PER + first, PER - first)], rrecv.at[q]).wait()
        rows = flat_rows(back[pl.ds(q * PER, PER)])
        at = lax.broadcasted_iota(I32, (TOK, TOK), 1) + q * TOK
        for k in range(2):
            part = dot((at == slot_col[k]).astype(F32).astype(BF), rows)
            if q == 0:
                pacc[k] = part
            elif q < CH - 1:
                pacc[k] = pacc[k] + part
            else:
                rows_o[k] = (pacc[k] + part).astype(BF)

    for q in range(CH - 1):
        gather(q)
    with jax.named_scope("lwait"):
        bytes_of(lback.at[pl.ds(1, NEP - 1)], lrecv).wait()

    scores = lback[...].reshape(NEP, 128).astype(BF)
    lane = lax.broadcasted_iota(I32, (TOK, 128), 1)
    down_i = lax.broadcasted_iota(I32, (128, 128), 0)
    over_i = lax.broadcasted_iota(I32, (128, 128), 1)
    logits = slog[...]
    keep = jnp.ones((TOK, 128), F32)
    for k in range(2):
        col = slot_col[k]
        kept = col >= 0
        spot = jnp.where(kept, col // 8, -1)
        mine = dot((lane == spot).astype(F32).astype(BF), scores)
        mine = jnp.where(lane // 16 == jnp.where(kept, col % 8, -1), mine, 0.0).astype(BF)
        spread = jnp.logical_and(down_i % 16 == over_i % 16, (over_i // 16) % 4 == k)
        logits = logits + dot(mine, spread.astype(F32).astype(BF))
        keep = jnp.where((lane // 16) % 4 == k, kept.astype(F32), keep)
    values = keep * jax.nn.sigmoid(logits)
    pair = values + pltpu.roll(values, 16, 1)
    weights = values / (pair + pltpu.roll(pair, 32, 1))
    wide = 4 * TB
    col = lax.broadcasted_iota(I32, (128, TASKS * wide), 1)
    line = lax.broadcasted_iota(I32, (128, TASKS * wide), 0)
    take = (line == (col % wide) // TB * 16 + col // wide).astype(F32).astype(BF)
    diagonal = (
        lax.broadcasted_iota(I32, (TOK, wide), 1) % TB == lax.broadcasted_iota(I32, (TOK, wide), 0) % TB
    )
    spread = dot(weights.astype(BF), take)
    for s in range(TASKS):
        w_o[s] = jnp.where(diagonal, spread[:, s * wide : (s + 1) * wide], 0.0).astype(BF)

    with jax.named_scope("owait"):
        result.wait()
    rows_o[3] = xrecv[...]
    gather(CH - 1)
    with jax.named_scope("sendwait"):
        bytes_of(wbuf.at[0, 0, pl.ds(1, 7)], zsend).wait()
        bytes_of(wbuf.at[0, pl.ds(1, 3)], ysend).wait()
        bytes_of(wbuf.at[0], csend).wait()
        bytes_of(tokq.at[pl.ds(1, 3)], tsend).wait()
        bytes_of(precv, psend).wait()
        bytes_of(snd.at[pl.ds(1, NEP - 1)], dsend).wait()
        bytes_of(lret.at[pl.ds(1, NEP - 1)], lsend).wait()
        bytes_of(ret.at[pl.ds(1, NEP - 1)], rsend).wait()


OUT_PARTS = 8


def mix(rows_r, w_r, out_h, buf, sem):
    size = TOK // OUT_PARTS

    def put(h):
        at = pl.ds(h * size, size)
        return pltpu.make_async_copy(buf.at[:, at], out_h.at[:, at], sem.at[h])

    for b in range(TOK // TB):
        at = slice(b * TB, (b + 1) * TB)
        terms = jnp.concatenate([rows_r[i, at] for i in range(4)], axis=0)
        left = jnp.concatenate([w_r[s, at] for s in range(TASKS)], axis=0)
        made = dot(left, terms).astype(BF)
        for s in range(TASKS):
            buf[s, at] = made[s * TB : (s + 1) * TB]
        if (b + 1) * TB % size == 0:
            put((b + 1) * TB // size - 1).start()
    for h in range(OUT_PARTS):
        put(h).wait()


def on_device(tokens, routes, capacity, expert_in, expert_out, shared_in, shared_out, route_gate, shared_gate):
    hbm = pl.BlockSpec(memory_space=pltpu.HBM)
    vmem = pl.BlockSpec(memory_space=pltpu.VMEM)
    dma = pltpu.SemaphoreType.DMA
    rows, weights = pl.pallas_call(
        exchange,
        out_shape=(
            jax.ShapeDtypeStruct((4, TOK, D), BF),
            jax.ShapeDtypeStruct((TASKS, TOK, 4 * TB), BF),
        ),
        in_specs=[hbm] * 9,
        out_specs=(vmem, vmem),
        scratch_shapes=[
            pltpu.VMEM((2, TOK), I32),
            pltpu.VMEM((1, NEP), I32),
            pltpu.VMEM((1, TASKS * D), BF),
            pltpu.VMEM((2, TASKS * D), BF),
            pltpu.VMEM((D, H), BF),
            pltpu.VMEM((H, D), BF),
            pltpu.VMEM((2, 2, 16, D), BF),
            pltpu.VMEM((2, 4, 8, 2, 16, D), BF),
            pltpu.VMEM((4, TOK, D), BF),
            pltpu.VMEM((NEP, 8, D), BF),
            pltpu.VMEM((NEP, 8, D), BF),
            pltpu.VMEM((NEP, 8, D), BF),
            pltpu.VMEM((NEP, 8, D), BF),
            pltpu.VMEM((NEP, 1, 128), F32),
            pltpu.VMEM((NEP, 1, 128), F32),
            pltpu.VMEM((4, TOK, D), F32),
            pltpu.VMEM((2, TOK, D), F32),
            pltpu.VMEM((TOK, D), BF),
            pltpu.VMEM((TOK, D), BF),
            pltpu.VMEM((2, TOK, D), F32),
            pltpu.VMEM((TOK, 128), F32),
            dma((6,)),
            dma((2,)),
            dma, dma((CH,)),
            dma, dma((CH,)),
            dma, dma,
            dma, dma((2,)),
            dma, dma,
            dma, dma((3,)),
            dma, dma((3,)),
            dma, dma((2,)),
            dma, dma,
            dma, dma((4,)),
        ],
        compiler_params=pltpu.CompilerParams(collective_id=0, has_side_effects=True, vmem_limit_bytes=40 * 2**20),
        name="exchange",
    )(*[
        pltpu.with_memory_space_constraint(a, pltpu.HBM)
        for a in (
            tokens, routes.T, capacity.reshape(1, NEP), expert_in, expert_out,
            shared_in, shared_out, route_gate, shared_gate,
        )
    ])
    mixed = pl.pallas_call(
        mix,
        out_shape=jax.ShapeDtypeStruct((TASKS, TOK, D), BF),
        in_specs=[vmem, vmem],
        out_specs=hbm,
        scratch_shapes=[pltpu.VMEM((TASKS, TOK, D), BF), dma((OUT_PARTS,))],
        compiler_params=pltpu.CompilerParams(vmem_limit_bytes=24 * 2**20),
        name="mix",
    )(rows, weights)
    return mixed.transpose(1, 0, 2)


def solution(mesh):
    rows, experts = P(("dp", "ep"), None), P("ep", None, None)
    return jax.shard_map(
        on_device,
        mesh=mesh,
        in_specs=(rows, rows, P(), experts, experts, P(None, "ep", None), P(None, "ep", None), P("ep", None), P()),
        out_specs=P(("dp", "ep"), None, None),
        check_vma=False,
    )
```
